32 devices in a mesh: rows: 8 (over z, y), mem: 4 (over x, core).
Axes of the slice: x: 2, y: 2, z: 4, core: 2. Of those that a mesh axis runs over, the one named last changes fastest.
Arguments:
- ensemble: float32 [64, 32, 48, 384], P('mem', None, 'rows'), may hold values from 0 to 2
- courant: float32 [3, 32, 48, 384], P(None, None, 'rows'), may hold values from -0.22 to 0.22
- obs_column: int32 [128], P('rows'), may hold values from 0 to 18431, as said below
- obs_value: float32 [32, 128], P(None, 'rows'), may hold values from -6 to 6
- obs_var: float32 [32, 128], P(None, 'rows'), may hold values from 0.5 to 8
Outputs:
- analysis: float32 [64, 32, 48, 384], P('mem', None, 'rows')
The draws below stay inside these ranges and needn't reach their ends.
Inputs may be any that keep to these rules, and one draw needn't show every extreme that they name: `obs_column`: entry p is x * 384 + y with x from (p // 16) * 6 to (p // 16) * 6 + 5.
All inputs are finite; a program needn't handle non-finite values.
Results may differ from the reference program's by a relative error of at most 0.0003.
Values sent between devices are 32-bit elements; how exact they have to be, the bound alone decides.
A program may use at most 128 MiB of HBM per device.

```python
import math
import jax
import jax.numpy as jnp
from jax import lax

ENSEMBLE_SIZE = 64
VERTICAL_COUNT = 32
ROW_CELLS = 384
RX = 6
PROF_DEV = 16
STEPS = 3
NS_ITERS = 4
GRID_ROWS = 48
NPROF = 128


def draw_obs_column(key, part):
    first_key, second_key = jax.random.split(jax.random.fold_in(key, 11))
    owner = jnp.arange(NPROF, dtype=jnp.int32) // PROF_DEV
    row_offset = jax.random.randint(first_key, (NPROF,), 0, RX, dtype=jnp.int32)
    column_y = jax.random.randint(second_key, (NPROF,), 0, ROW_CELLS, dtype=jnp.int32)
    return ((owner * RX + row_offset) * ROW_CELLS + column_y).astype(jnp.int32)


def block_levels(rng, extent, pieces, low, largest):
    loudness, own = 1.0, jax.random.fold_in(rng, 6)
    for dim, parts in pieces:
        heights = jnp.exp(jax.random.uniform(jax.random.fold_in(own, dim), (parts,), jnp.float32, low / len(pieces), largest / len(pieces)))
        loudness = loudness * jnp.repeat(heights, extent[dim] // parts).reshape([-1 if axis == dim else 1 for axis in range(len(extent))])
    return loudness


def bell_draw(key, extent, spread, limit, cuts=(), held_as=jnp.bfloat16):
    drawn = spread * jax.random.normal(key, extent, jnp.float32)
    if cuts:
        drawn = drawn * block_levels(key, extent, cuts, -0.22, 0.18)
    return jnp.clip(drawn, -limit, limit).astype(held_as)


def setup_inputs(seed: int = 0) -> dict:
    key_list = jax.random.split(jax.random.key(seed), 6)
    ensemble = jnp.clip(2.0 * jax.random.uniform(key_list[0], (ENSEMBLE_SIZE, VERTICAL_COUNT, GRID_ROWS, ROW_CELLS), jnp.float32) ** block_levels(key_list[0], (ENSEMBLE_SIZE, VERTICAL_COUNT, GRID_ROWS, ROW_CELLS), ((0, 4), (2, 8)), -0.2, 0.2), 0.0, 2.0)
    courant = jnp.clip(jax.random.uniform(key_list[1], (3, VERTICAL_COUNT, GRID_ROWS, ROW_CELLS), jnp.float32, -0.22, 0.22) * block_levels(key_list[1], (3, VERTICAL_COUNT, GRID_ROWS, ROW_CELLS), ((2, 8),), -0.4, 0.0), -0.22, 0.22)
    obs_column = draw_obs_column(jax.random.fold_in(key_list[5], 71), 0)
    obs_value = bell_draw(key_list[3], (VERTICAL_COUNT, NPROF), 1.0, 6.0, ((1, 8),), jnp.float32)
    obs_var = jnp.clip(jnp.exp(math.log(8.0) - 2.7725887 * jax.random.uniform(key_list[4], (VERTICAL_COUNT, NPROF), jnp.float32) ** block_levels(key_list[4], (VERTICAL_COUNT, NPROF), ((1, 8),), -0.2, 0.2)), 0.5, 8.0)
    return {"ensemble": ensemble, "courant": courant, "obs_column": obs_column, "obs_value": obs_value, "obs_var": obs_var}


DIFFUSION = 0.05

def advance(padded, courant):
    center = padded[:, :, 1:-1, :]
    below_x = padded[:, :, :-2, :]
    above_x = padded[:, :, 2:, :]
    padded_y = jnp.pad(center, ((0, 0), (0, 0), (0, 0), (1, 1)))
    below_y = padded_y[:, :, :, :-2]
    above_y = padded_y[:, :, :, 2:]
    padded_z = jnp.pad(center, ((0, 0), (1, 1), (0, 0), (0, 0)))
    below_z = padded_z[:, :-2]
    above_z = padded_z[:, 2:]
    change = jnp.zeros_like(center)
    for component, below, above in ((0, below_x, above_x), (1, below_y, above_y), (2, below_z, above_z)):
        velocity = courant[component][None]
        change = change - jnp.maximum(velocity, 0.0) * (center - below) - jnp.minimum(velocity, 0.0) * (above - center) + DIFFUSION * (above + below - 2.0 * center)
    return center + change

def gram_terms(profiles, obs_value, obs_var):
    members_all = profiles.shape[0]
    center = lax.optimization_barrier(jnp.mean(profiles, axis=0))
    scaling = 1.0 / jnp.sqrt((members_all - 1.0) * obs_var)
    scaled = ((profiles - center[None]) * scaling[None]).reshape(members_all, -1)
    innovation = ((obs_value - center) / jnp.sqrt(obs_var)).reshape(-1)
    gram_part = jnp.dot(scaled, scaled.T, precision=lax.Precision.HIGHEST)
    pull_part = jnp.dot(scaled, innovation, precision=lax.Precision.HIGHEST)
    return (gram_part, pull_part)

def mixing(gram_sum, pull_sum):
    members_all = gram_sum.shape[0]
    identity_matrix = jnp.eye(members_all, dtype=jnp.float32)
    system = identity_matrix + gram_sum
    frobenius = jnp.sqrt(jnp.sum(system * system))

    def newton(iteration, carry):
        iterate, inverse_root = carry
        factor = 0.5 * (3.0 * identity_matrix - jnp.dot(inverse_root, iterate, precision=lax.Precision.HIGHEST))
        return (jnp.dot(iterate, factor, precision=lax.Precision.HIGHEST), jnp.dot(factor, inverse_root, precision=lax.Precision.HIGHEST))
    iterate, inverse_root = lax.fori_loop(0, NS_ITERS, newton, (system / frobenius, identity_matrix))
    root_inverse = inverse_root / jnp.sqrt(frobenius)
    mean_shift = jnp.dot(root_inverse, jnp.dot(root_inverse, pull_sum, precision=lax.Precision.HIGHEST), precision=lax.Precision.HIGHEST) / jnp.sqrt(members_all - 1.0)
    centering = identity_matrix - 1.0 / members_all
    return 1.0 / members_all + jnp.dot(centering, mean_shift[:, None] + root_inverse, precision=lax.Precision.HIGHEST)

def reference(ensemble, courant, obs_column, obs_value, obs_var):

    def prior_state(member_index):
        concentration = member_index[None]
        for counter in range(STEPS):
            padded = jnp.pad(concentration, ((0, 0), (0, 0), (1, 1), (0, 0)))
            concentration = advance(padded, courant)
        return concentration[0]
    prior_states = lax.map(prior_state, ensemble)
    state_vectors = prior_states.reshape(ENSEMBLE_SIZE, VERTICAL_COUNT, GRID_ROWS * ROW_CELLS)
    profiles = jnp.take(state_vectors, obs_column, axis=2)
    gram_sum, pull_sum = gram_terms(profiles, obs_value, obs_var)
    transform_weights = mixing(gram_sum, pull_sum)
    updated_ensemble = jnp.dot(transform_weights.T, prior_states.reshape(ENSEMBLE_SIZE, -1), precision=lax.Precision.HIGHEST)
    return updated_ensemble.reshape(ensemble.shape)
```

```python
import functools

import jax
import jax.numpy as jnp
from jax import lax
from jax.experimental import pallas as pl
from jax.experimental.pallas import tpu as pltpu
from jax.sharding import PartitionSpec as P

NS_ITERS = 4
DIFFUSION = 0.05
AHEAD = 2
LAG = 2
LANES = 128
TILE = 8
MESH = pl.DeviceIdType.MESH
HIGHEST = lax.Precision.HIGHEST


def cdiv(a, b):
    return -(-a // b)


def kernel(
    rows_n, mem_n,
    ens_any, cour_any, obs, obs_value, obs_var,
    out,
    ens, cour, chalo, chalo3, hal, coef, cext, w0, w1, w2, z0, z1, z2, z3, fc,
    obsv, hot, pp, prec, prof, scal, grec, gall, wts, wsp,
    e_load, c_load,
    c_send, c_recv, cf_send, cf_recv, d_send, d_recv, df_send, df_recv, o_send, o_recv,
    h_send, h_recv,
    x_send, p_send, f_recv, r_send, r_recv, q_send, q_recv, g_send, g_recv, a_send, a_recv,
):
    members, rows, levels, width = ens.shape
    total = members * mem_n
    nobs = obs.shape[0]
    chips = mem_n // 2
    groups = levels // TILE
    row = lax.axis_index("rows")
    mem = lax.axis_index("mem")
    core = lax.rem(mem, 2)
    chip = mem // 2
    partner = chip * 2 + 1 - core
    f32 = jnp.float32

    def remote(src, dst, ssem, rsem, r, m):
        return pltpu.make_async_remote_copy(
            src_ref=src, dst_ref=dst, send_sem=ssem, recv_sem=rsem,
            device_id=(r, m), device_id_type=MESH,
        )

    def load_cour():
        return pltpu.make_async_copy(cour_any, cour, c_load.at[0])

    def load_ens(m):
        return pltpu.make_async_copy(ens_any.at[m], ens.at[m], e_load.at[m])

    load_cour().start()

    @pl.loop(0, members)
    def _(m):
        load_ens(m).start()

    barrier = pltpu.get_barrier_semaphore()
    for d in range(1, mem_n):
        pl.semaphore_signal(barrier, inc=1, device_id=(row, lax.rem(mem + d, mem_n)), device_id_type=MESH)
    for d in range(1, rows_n):
        pl.semaphore_signal(barrier, inc=1, device_id=(lax.rem(row + d, rows_n), mem), device_id_type=MESH)

    has_low = row > 0
    has_high = row < rows_n - 1
    low = jnp.maximum(row - 1, 0)
    high = jnp.minimum(row + 1, rows_n - 1)

    lane = lax.broadcasted_iota(jnp.int32, (TILE, LANES), 1)
    slot = lax.rem(lane, nobs)
    ox = jnp.zeros((TILE, LANES), jnp.int32)
    oy = jnp.zeros((TILE, LANES), jnp.int32)
    for p in range(nobs):
        gx = lax.div(obs[p], width)
        ox = jnp.where(slot == p, gx, ox)
        oy = jnp.where(slot == p, obs[p] - gx * width, oy)
    obsv[0, 0] = ox
    obsv[0, 1] = oy

    load_cour().wait()
    load_ens(0).wait()
    pl.semaphore_wait(barrier, mem_n - 1 + rows_n - 1)

    def chalo_up():
        return remote(cour.at[:, rows - 2 + core], chalo.at[0, core], c_send.at[0], c_recv.at[0], high, mem)

    def chalo_down():
        return remote(cour.at[:, core], chalo.at[1, core], c_send.at[1], c_recv.at[1], low, mem)

    def chalo_pass(side):
        return remote(chalo.at[side, core], chalo.at[side, core], cf_send.at[side], cf_recv.at[side], row, partner)

    def far_up():
        return remote(cour.at[0, rows - 3], chalo3.at[0], d_send.at[0], d_recv.at[0], high, mem)

    def far_down():
        return remote(cour.at[0, 2], chalo3.at[1], d_send.at[1], d_recv.at[1], low, mem)

    def far_pass(side):
        return remote(chalo3.at[side], chalo3.at[side], df_send.at[side], df_recv.at[side], row, partner)

    def obs_up():
        return remote(obsv.at[0], obsv.at[1], o_send.at[0], o_recv.at[0], high, mem)

    def obs_down():
        return remote(obsv.at[0], obsv.at[2], o_send.at[1], o_recv.at[1], low, mem)

    def halo_up(m):
        return remote(ens.at[m, pl.ds(rows - 3, 3)], hal.at[m, 0], h_send.at[0, m], h_recv.at[0, m], high, mem)

    def halo_down(m):
        return remote(ens.at[m, pl.ds(0, 3)], hal.at[m, 1], h_send.at[1, m], h_recv.at[1, m], low, mem)

    first = core == 0

    @pl.when(has_high)
    def _():
        chalo_up().start()

    @pl.when(has_low)
    def _():
        chalo_down().start()

    def send_halo(m):
        @pl.when(has_high)
        def _():
            halo_up(m).start()

        @pl.when(has_low)
        def _():
            halo_down(m).start()

    send_halo(0)

    @pl.when(has_high)
    def _():
        obs_up().start()

        @pl.when(first)
        def _():
            far_up().start()

    @pl.when(has_low)
    def _():
        obs_down().start()

        @pl.when(first)
        def _():
            far_down().start()

    ahead = min(AHEAD, members)

    @pl.loop(1, members)
    def _(m):
        load_ens(m).wait()

    @pl.loop(1, ahead)
    def _(m):
        send_halo(m)

    level = lax.broadcasted_iota(jnp.int32, (levels, width), 0)
    cell = lax.broadcasted_iota(jnp.int32, (levels, width), 1)

    def set_coef(i, a0, a1, a2):
        coef[i, 0] = 1.0 - 6.0 * DIFFUSION - jnp.abs(a0) - jnp.abs(a1) - jnp.abs(a2)
        coef[i, 1] = DIFFUSION + jnp.maximum(a0, 0.0)
        coef[i, 2] = DIFFUSION - jnp.minimum(a0, 0.0)
        coef[i, 3] = jnp.where(cell > 0, DIFFUSION + jnp.maximum(a1, 0.0), 0.0)
        coef[i, 4] = jnp.where(cell < width - 1, DIFFUSION - jnp.minimum(a1, 0.0), 0.0)
        coef[i, 5] = jnp.where(level > 0, DIFFUSION + jnp.maximum(a2, 0.0), 0.0)
        coef[i, 6] = jnp.where(level < levels - 1, DIFFUSION - jnp.minimum(a2, 0.0), 0.0)

    @pl.loop(0, rows)
    def _(i):
        set_coef(i + 2, cour[0, i], cour[1, i], cour[2, i])

    def clear(ref, start, count):
        ref[pl.ds(start, count)] = jnp.zeros((count, levels, width), f32)

    @pl.loop(0, members)
    def _(m):
        out[m] = jnp.zeros((rows, levels, width), f32)

    clear(z0, 0, 1)
    clear(z0, rows + 1, 1)
    clear(z1, 0, 1)
    clear(z1, rows + 3, 1)
    clear(z2, 0, 1)
    clear(z2, rows + 5, 1)

    @pl.when(jnp.logical_not(has_low))
    def _():
        clear(w0, 0, 3)
        coef[pl.ds(0, 2)] = jnp.zeros((2, 7, levels, width), f32)
        cext[0] = jnp.zeros((levels, width), f32)
        obsv[1] = jnp.full((2, TILE, LANES), -1, jnp.int32)
        prec[0] = jnp.zeros((groups, members, LANES), f32)

    @pl.when(jnp.logical_not(has_high))
    def _():
        clear(w0, rows + 3, 3)
        coef[pl.ds(rows + 2, 2)] = jnp.zeros((2, 7, levels, width), f32)
        cext[1] = jnp.zeros((levels, width), f32)
        obsv[2] = jnp.full((2, TILE, LANES), -1, jnp.int32)
        prec[1] = jnp.zeros((groups, members, LANES), f32)

    def edge(side, present, begin):
        @pl.when(present)
        def _():
            (chalo_down if side else chalo_up)().wait_recv()
            chalo_pass(side).start()
            (obs_down if side else obs_up)().wait_recv()

            @pl.when(first)
            def _():
                (far_down if side else far_up)().wait_recv()
                far_pass(side).start()

            @pl.when(jnp.logical_not(first))
            def _():
                far_pass(side).wait_recv()

            chalo_pass(side).wait_recv()

            @pl.loop(0, 2)
            def _(i):
                set_coef(begin + i, chalo[side, i, 0], chalo[side, i, 1], chalo[side, i, 2])

            a0 = chalo3[side]
            cext[side] = DIFFUSION + (jnp.maximum(a0, 0.0) if side else -jnp.minimum(a0, 0.0))

    edge(0, has_low, 0)
    edge(1, has_high, rows + 2)

    for k in range(3):
        hot[k] = jnp.where(
            lax.broadcasted_iota(jnp.int32, (width, LANES), 0) == obsv[k, 1, :1], 1.0, 0.0
        ).astype(jnp.bfloat16)

    def update(src, i, c):
        mid = src[i + 1]
        return (
            coef[c, 0] * mid
            + coef[c, 1] * src[i]
            + coef[c, 2] * src[i + 2]
            + coef[c, 3] * pltpu.roll(mid, 1, 1)
            + coef[c, 4] * pltpu.roll(mid, width - 1, 1)
            + coef[c, 5] * pltpu.roll(mid, 1, 0)
            + coef[c, 6] * pltpu.roll(mid, levels - 1, 0)
        )

    def other(d):
        return lax.rem(chip + d, chips) * 2 + core

    def send_x(d, m):
        slot = fc.at[mem * members + m]
        return remote(slot, slot, x_send.at[d, m], f_recv.at[mem, m], row, other(d))

    def send_p(d, m):
        src = lax.rem(chip + d, chips) * 2 + core
        slot = fc.at[src * members + m]
        return remote(slot, slot, p_send.at[d, m], f_recv.at[src, m], row, partner)

    def arrived(src, m):
        slot = fc.at[src * members + m]
        return remote(slot, slot, p_send.at[0, 0], f_recv.at[src, m], row, partner)

    def forward(m):
        for d in range(1, chips):
            arrived(other(d), m).wait_recv()
            send_p(d, m).start()

    def service(m):
        @pl.when(has_low)
        def _():
            halo_up(m).wait_recv()
            w0[pl.ds(0, 3)] = hal[m, 0]

        @pl.when(has_high)
        def _():
            halo_down(m).wait_recv()
            w0[pl.ds(rows + 3, 3)] = hal[m, 1]

        @pl.when(m + ahead < members)
        def _():
            send_halo(m + ahead)

        w0[pl.ds(3, rows)] = ens[m]

        @pl.loop(0, rows + 4, unroll=2)
        def _(i):
            w1[i] = update(w0, i, i)

        @pl.loop(0, rows + 2, unroll=2)
        def _(i):
            w2[i] = update(w1, i, i + 1)

        @pl.loop(0, rows, unroll=2)
        def _(i):
            fc[mem * members + m, i] = update(w2, i, i + 2)

        for d in range(1, chips):
            send_x(d, m).start()
        send_p(0, m).start()

        @pl.when(m >= LAG)
        def _():
            forward(m - LAG)

    inside = lax.broadcasted_iota(jnp.int32, (levels, LANES), 0)
    owner = lax.broadcasted_iota(jnp.int32, (levels, LANES), 1) // nobs
    pick = lax.rem(inside, TILE) == owner

    def fold(x):
        return jnp.sum(jnp.where(pick, x, 0.0).reshape(groups, TILE, LANES), axis=1)

    def profile(m):
        z0[pl.ds(1, rows)] = ens[m]
        z1[1] = coef[1, 2] * z0[1]
        z1[rows + 2] = coef[rows + 2, 1] * z0[rows]

        @pl.loop(0, rows, unroll=2)
        def _(i):
            z1[i + 2] = update(z0, i, i + 2)

        z2[1] = coef[0, 2] * z1[1]
        z2[rows + 4] = coef[rows + 3, 1] * z1[rows + 2]

        @pl.loop(0, rows + 2, unroll=2)
        def _(i):
            z2[i + 2] = update(z1, i, i + 1)

        z3[0] = cext[0] * z2[1]
        z3[rows + 5] = cext[1] * z2[rows + 4]

        @pl.loop(0, rows + 4, unroll=2)
        def _(i):
            z3[i + 1] = update(z2, i, i)

        for k, begin, count in ((0, 3, rows), (1, 0, 3), (2, rows + 3, 3)):
            x = z3[pl.ds(begin, count)].reshape(count * levels, width)
            high_part = x.astype(jnp.bfloat16)
            low_part = (x - high_part.astype(f32)).astype(jnp.bfloat16)
            got = jnp.dot(high_part, hot[k], preferred_element_type=f32)
            got = got + jnp.dot(low_part, hot[k], preferred_element_type=f32)
            at = obsv[k, 0, :1] - row * rows + 3
            acc = jnp.zeros((levels, LANES), f32)
            for i in range(count):
                acc = acc + jnp.where(at == begin + i, got[i * levels:(i + 1) * levels], 0.0)
            pp[k, :, pl.ds(m, 1)] = fold(acc)[:, None]

    def dot(a, b):
        return jnp.dot(a, b, precision=HIGHEST, preferred_element_type=f32)

    mine = pl.ds(pl.multiple_of(mem * members, members), members)

    def give_low():
        return remote(pp.at[1], prec.at[1], r_send.at[1], r_recv.at[1], low, mem)

    def give_high():
        return remote(pp.at[2], prec.at[0], r_send.at[0], r_recv.at[0], high, mem)

    def stage_a():
        @pl.when(has_high)
        def _():
            give_high().start()

        @pl.when(has_low)
        def _():
            give_low().start()

    def give_prof(d):
        block = prof.at[:, mine]
        return remote(block, block, q_send.at[d], q_recv.at[mem], row, lax.rem(mem + d, mem_n))

    def stage_b():
        @pl.when(has_low)
        def _():
            give_high().wait_recv()

        @pl.when(has_high)
        def _():
            give_low().wait_recv()

        prof[:, mine] = pp[0] + prec[0] + prec[1]
        for d in range(1, mem_n):
            give_prof(d).start()

    def flat(ref):
        repeat = lax.broadcasted_iota(jnp.int32, (nobs, LANES), 1) % nobs
        repeat = jnp.where(repeat == lax.broadcasted_iota(jnp.int32, (nobs, LANES), 0), 1.0, 0.0).astype(f32)
        got = fold(dot(ref[...].T, repeat))
        return jnp.concatenate([got[q:q + 1] for q in range(groups)], axis=1)

    def give_gram(d):
        return remote(grec.at[row], grec.at[row], g_send.at[d], g_recv.at[row], lax.rem(row + d, rows_n), mem)

    def stage_c():
        for d in range(1, mem_n):
            src = lax.rem(mem + d, mem_n)
            block = prof.at[:, pl.ds(pl.multiple_of(src * members, members), members)]
            remote(block, block, q_send.at[d], q_recv.at[src], row, src).wait_recv()
        values = jnp.concatenate([prof[q] for q in range(groups)], axis=1)
        variance = flat(obs_var)
        center = jnp.mean(values, axis=0, keepdims=True)
        scaled = (values - center) / jnp.sqrt((total - 1.0) * variance)
        innovation = (flat(obs_value) - center) / jnp.sqrt(variance)
        pad = jnp.broadcast_to(innovation, (LANES - total, innovation.shape[1]))
        scal[...] = scaled
        both = jnp.concatenate([scaled, pad], axis=0)
        grec[row] = lax.dot_general(
            scal[mine], both, (((1,), (1,)), ((), ())), precision=HIGHEST, preferred_element_type=f32
        )
        for d in range(1, rows_n):
            give_gram(d).start()

    def give_sum(d):
        return remote(gall.at[mine], gall.at[mine], a_send.at[d], a_recv.at[mem], row, lax.rem(mem + d, mem_n))

    def stage_d():
        for d in range(1, rows_n):
            src = lax.rem(row + d, rows_n)
            remote(grec.at[src], grec.at[src], g_send.at[d], g_recv.at[src], src, mem).wait_recv()
        part = grec[0]
        for r in range(1, rows_n):
            part = part + grec[r]
        gall[mine] = part
        for d in range(1, mem_n):
            give_sum(d).start()

    def stage_e():
        for d in range(1, mem_n):
            src = lax.rem(mem + d, mem_n)
            block = gall.at[pl.ds(pl.multiple_of(src * members, members), members)]
            remote(block, block, a_send.at[d], a_recv.at[src], row, src).wait_recv()
        gsum = gall[...]
        ri = lax.broadcasted_iota(jnp.int32, (total, total), 0)
        ci = lax.broadcasted_iota(jnp.int32, (total, total), 1)
        eye = jnp.where(ri == ci, 1.0, 0.0).astype(f32)
        system = eye + gsum[:, :total]
        frob = jnp.sqrt(jnp.sum(jnp.sum(system * system, axis=1, keepdims=True), axis=0, keepdims=True))
        y = system / frob
        z = eye
        for it in range(NS_ITERS):
            factor = 0.5 * (3.0 * eye - (y if it == 0 else dot(z, y)))
            if it < NS_ITERS - 1:
                y = dot(y, factor)
            z = factor if it == 0 else dot(factor, z)
        root = z / jnp.sqrt(frob)
        shift = dot(root, dot(root, gsum))[:, total:total + 1] / jnp.sqrt(f32(total - 1.0))
        mixed = shift + root
        weights = 1.0 / total + mixed - jnp.mean(mixed, axis=0, keepdims=True)
        wts[...] = weights.T
        own = wts[mine].T
        for k in range(members):
            wsp[k] = jnp.broadcast_to(own[:, k:k + 1], (total, LANES))

    block = min(4, members)
    tiles = width // LANES

    def mix(m):
        for d in range(chips):
            arrived(lax.rem(chip + d, chips) * 2 + 1 - core, m).wait_recv()

        @pl.loop(0, members // block)
        def _(b):
            ws = [
                [
                    jnp.broadcast_to(wsp[b * block + k, pl.ds(s * members + m, 1)], (TILE, LANES))
                    for s in range(mem_n)
                ]
                for k in range(block)
            ]

            @pl.loop(0, rows)
            def _(i):
                for t in range(groups):
                    for c in range(tiles):
                        at = (i, pl.ds(t * TILE, TILE), pl.ds(c * LANES, LANES))
                        f = [fc[(s * members + m,) + at] for s in range(mem_n)]
                        for k in range(block):
                            acc = out[(b * block + k,) + at]
                            for s in range(mem_n):
                                acc = acc + ws[k][s] * f[s]
                            out[(b * block + k,) + at] = acc

    passes = min(4, members)
    per_pass = cdiv(members, passes)
    gap = max(1, (members - passes) // 6)
    at_a = passes - 1
    at_b, at_c, at_d, at_e = (at_a + gap * n for n in range(1, 5))
    per_mix = 3
    mixed_in_loop = max(0, members - 1 - at_e) * per_mix
    assert at_e < members and mixed_in_loop <= members - LAG

    @pl.loop(0, members)
    def _(m):
        service(m)

        @pl.when(m < passes)
        def _():
            @pl.loop(0, per_pass)
            def _(n):
                profile(m * per_pass + n)

        for at, stage in ((at_a, stage_a), (at_b, stage_b), (at_c, stage_c), (at_d, stage_d), (at_e, stage_e)):
            pl.when(m == at)(stage)

        @pl.when(m > at_e)
        def _():
            @pl.loop(0, per_mix)
            def _(n):
                mix((m - at_e - 1) * per_mix + n)

    @pl.loop(members - LAG, members)
    def _(m):
        forward(m)

    @pl.loop(mixed_in_loop, members)
    def _(m):
        mix(m)

    @pl.when(has_high)
    def _():
        chalo_up().wait_send()
        chalo_pass(1).wait_send()
        obs_up().wait_send()
        give_high().wait_send()

        @pl.when(first)
        def _():
            far_up().wait_send()
            far_pass(1).wait_send()

    @pl.when(has_low)
    def _():
        chalo_down().wait_send()
        chalo_pass(0).wait_send()
        obs_down().wait_send()
        give_low().wait_send()

        @pl.when(first)
        def _():
            far_down().wait_send()
            far_pass(0).wait_send()

    @pl.loop(0, members)
    def _(m):
        @pl.when(has_high)
        def _():
            halo_up(m).wait_send()

        @pl.when(has_low)
        def _():
            halo_down(m).wait_send()

        for d in range(1, chips):
            send_x(d, m).wait_send()
        for d in range(chips):
            send_p(d, m).wait_send()

    for d in range(1, mem_n):
        give_prof(d).wait_send()
        give_sum(d).wait_send()
    for d in range(1, rows_n):
        give_gram(d).wait_send()


def per_device(rows_n, mem_n, ensemble, courant, obs_column, obs_value, obs_var):
    members, levels, rows, width = ensemble.shape
    nobs = obs_column.shape[0]
    chips = mem_n // 2
    groups = levels // TILE
    f32 = jnp.float32
    vmem = pl.BlockSpec(memory_space=pltpu.VMEM)
    smem = pl.BlockSpec(memory_space=pltpu.SMEM)
    hbm = pl.BlockSpec(memory_space=pl.ANY)
    dma = pltpu.SemaphoreType.DMA
    total = members * mem_n
    plane = (levels, width)
    result = pl.pallas_call(
        functools.partial(kernel, rows_n, mem_n),
        out_shape=pltpu.VMEM((members, rows) + plane, f32),
        in_specs=[hbm, hbm, smem, vmem, vmem],
        out_specs=vmem,
        scratch_shapes=[
            pltpu.VMEM((members, rows) + plane, f32),
            pltpu.VMEM((3, rows) + plane, f32),
            pltpu.VMEM((2, 2, 3) + plane, f32),
            pltpu.VMEM((2,) + plane, f32),
            pltpu.VMEM((members, 2, 3) + plane, f32),
            pltpu.VMEM((rows + 4, 7) + plane, f32),
            pltpu.VMEM((2,) + plane, f32),
            pltpu.VMEM((rows + 6,) + plane, f32),
            pltpu.VMEM((rows + 4,) + plane, f32),
            pltpu.VMEM((rows + 2,) + plane, f32),
            pltpu.VMEM((rows + 2,) + plane, f32),
            pltpu.VMEM((rows + 4,) + plane, f32),
            pltpu.VMEM((rows + 6,) + plane, f32),
            pltpu.VMEM((rows + 6,) + plane, f32),
            pltpu.VMEM((total, rows) + plane, f32),
            pltpu.VMEM((3, 2, TILE, LANES), jnp.int32),
            pltpu.VMEM((3, width, LANES), jnp.bfloat16),
            pltpu.VMEM((3, groups, members, LANES), f32),
            pltpu.VMEM((2, groups, members, LANES), f32),
            pltpu.VMEM((groups, total, LANES), f32),
            pltpu.VMEM((total, groups * LANES), f32),
            pltpu.VMEM((rows_n, members, LANES), f32),
            pltpu.VMEM((total, LANES), f32),
            pltpu.VMEM((total, total), f32),
            pltpu.VMEM((members, total, LANES), f32),
            dma((members,)), dma((1,)),
            dma((2,)), dma((2,)), dma((2,)), dma((2,)),
            dma((2,)), dma((2,)), dma((2,)), dma((2,)), dma((2,)), dma((2,)),
            dma((2, members)), dma((2, members)),
            dma((chips, members)), dma((chips, members)), dma((mem_n, members)),
            dma((2,)), dma((2,)),
            dma((mem_n,)), dma((mem_n,)),
            dma((rows_n,)), dma((rows_n,)),
            dma((mem_n,)), dma((mem_n,)),
        ],
        compiler_params=pltpu.CompilerParams(
            collective_id=0, has_side_effects=True, vmem_limit_bytes=52 * 1024 * 1024
        ),
    )(
        ensemble.transpose(0, 2, 1, 3),
        courant.transpose(0, 2, 1, 3),
        obs_column,
        obs_value.T,
        obs_var.T,
    )
    return result.transpose(0, 2, 1, 3)


def solution(mesh):
    return jax.shard_map(
        functools.partial(per_device, mesh.shape["rows"], mesh.shape["mem"]),
        mesh=mesh,
        in_specs=(
            P("mem", None, "rows", None),
            P(None, None, "rows", None),
            P("rows"),
            P(None, "rows"),
            P(None, "rows"),
        ),
        out_specs=P("mem", None, "rows", None),
        check_vma=False,
    )
```

```python
import functools

import jax
import jax.numpy as jnp
from jax import lax
from jax.experimental import pallas as pl
from jax.experimental.pallas import tpu as pltpu
from jax.sharding import PartitionSpec as P

NS_ITERS = 4
DIFFUSION = 0.05
NEAR = 2
FAR = 1
DETOUR = 3
RELAY = 1
LAG = 2
PER_PASS = 4
STAGES = (2, 4, 6, 6)
PER_MIX = 3
LANES = 128
TILE = 8
MESH = pl.DeviceIdType.MESH
HIGHEST = lax.Precision.HIGHEST


def kernel(
    rows_n, mem_n,
    ens_any, cour_any, obs, obs_value, obs_var,
    out,
    ens, cour, chalo, chalo3, hal, coef, cext, w1, w2, z1, z2, zb, rbuf, fc,
    obsv, hot, pp, prec, prof, scal, grec, gall, wts, wsp,
    e_load, c_load,
    c_send, c_recv, cf_send, cf_recv, d_send, d_recv, df_send, df_recv, o_send, o_recv,
    h_send, h_recv, rb_recv, rf_send,
    x_send, p_send, f_recv, r_send, r_recv, q_send, q_recv, g_send, g_recv, a_send, a_recv,
):
    members, rows, levels, width = ens.shape
    total = members * mem_n
    nobs = obs.shape[0]
    chips = mem_n // 2
    groups = levels // TILE
    row = lax.axis_index("rows")
    mem = lax.axis_index("mem")
    core = lax.rem(mem, 2)
    chip = mem // 2
    partner = chip * 2 + 1 - core
    f32 = jnp.float32

    def remote(src, dst, ssem, rsem, r, m):
        return pltpu.make_async_remote_copy(
            src_ref=src, dst_ref=dst, send_sem=ssem, recv_sem=rsem,
            device_id=(r, m), device_id_type=MESH,
        )

    def load_cour():
        return pltpu.make_async_copy(cour_any, cour, c_load.at[0])

    def load_ens(m):
        return pltpu.make_async_copy(ens_any.at[m], ens.at[m], e_load.at[m])

    load_cour().start()

    @pl.loop(0, members)
    def _(m):
        load_ens(m).start()

    barrier = pltpu.get_barrier_semaphore()
    for d in range(1, mem_n):
        pl.semaphore_signal(barrier, inc=1, device_id=(row, lax.rem(mem + d, mem_n)), device_id_type=MESH)
    for d in range(1, rows_n):
        pl.semaphore_signal(barrier, inc=1, device_id=(lax.rem(row + d, rows_n), mem), device_id_type=MESH)

    has_low = row > 0
    has_high = row < rows_n - 1
    low = jnp.maximum(row - 1, 0)
    high = jnp.minimum(row + 1, rows_n - 1)

    lane = lax.broadcasted_iota(jnp.int32, (TILE, LANES), 1)
    slot = lax.rem(lane, nobs)
    ox = jnp.zeros((TILE, LANES), jnp.int32)
    oy = jnp.zeros((TILE, LANES), jnp.int32)
    for p in range(nobs):
        gx = lax.div(obs[p], width)
        ox = jnp.where(slot == p, gx, ox)
        oy = jnp.where(slot == p, obs[p] - gx * width, oy)
    obsv[0, 0] = ox
    obsv[0, 1] = oy

    load_cour().wait()
    load_ens(0).wait()
    pl.semaphore_wait(barrier, mem_n - 1 + rows_n - 1)

    def chalo_up():
        return remote(cour.at[:, rows - 2 + core], chalo.at[0, core], c_send.at[0], c_recv.at[0], high, mem)

    def chalo_down():
        return remote(cour.at[:, core], chalo.at[1, core], c_send.at[1], c_recv.at[1], low, mem)

    def chalo_pass(side):
        return remote(chalo.at[side, core], chalo.at[side, core], cf_send.at[side], cf_recv.at[side], row, partner)

    def far_up():
        return remote(cour.at[0, rows - 3], chalo3.at[0], d_send.at[0], d_recv.at[0], high, mem)

    def far_down():
        return remote(cour.at[0, 2], chalo3.at[1], d_send.at[1], d_recv.at[1], low, mem)

    def far_pass(side):
        return remote(chalo3.at[side], chalo3.at[side], df_send.at[side], df_recv.at[side], row, partner)

    def obs_up():
        return remote(obsv.at[0], obsv.at[1], o_send.at[0], o_recv.at[0], high, mem)

    def obs_down():
        return remote(obsv.at[0], obsv.at[2], o_send.at[1], o_recv.at[1], low, mem)

    def halo_up(m):
        return remote(ens.at[m, pl.ds(rows - 3, 3)], hal.at[m, 0], h_send.at[0, m], h_recv.at[0, m], high, mem)

    def halo_down(m):
        return remote(ens.at[m, pl.ds(0, 3)], hal.at[m, 1], h_send.at[1, m], h_recv.at[1, m], low, mem)

    first = core == 0

    odd = lax.rem(row, 2) == 1
    ahead_up = jnp.where(odd, FAR, NEAR)
    ahead_down = jnp.where(odd, NEAR, FAR)

    pairs = max(1, rows_n // 2)
    pair = row // 2
    send_limit = jnp.where(odd, pair, pairs - 1 - pair)
    relay_limit = jnp.where(odd, pairs - 1 - pair, pair)
    relay_side = jnp.where(odd, 1, 0)
    relay_on = jnp.logical_and(jnp.where(odd, row - 2, row) >= 0, jnp.where(odd, row, row + 2) < rows_n)
    relay_row = jnp.clip(jnp.where(odd, row - 2, row + 2), 0, rows_n - 1)

    def detour(m):
        return jnp.logical_and(lax.rem(m, pairs) > send_limit, jnp.logical_and(has_low, has_high))

    def send_up(m):
        @pl.when(jnp.logical_and(has_high, jnp.logical_not(jnp.logical_and(odd, detour(m)))))
        def _():
            halo_up(m).start()

    def send_down(m):
        @pl.when(jnp.logical_and(has_low, jnp.logical_or(odd, jnp.logical_not(detour(m)))))
        def _():
            halo_down(m).start()

    def send_detour(m):
        @pl.when(jnp.logical_and(odd, detour(m)))
        def _():
            remote(ens.at[m, pl.ds(rows - 3, 3)], rbuf.at[m], h_send.at[0, m], rb_recv.at[m], low, mem).start()

        @pl.when(jnp.logical_and(jnp.logical_not(odd), detour(m)))
        def _():
            remote(ens.at[m, pl.ds(0, 3)], rbuf.at[m], h_send.at[1, m], rb_recv.at[m], high, mem).start()

    def relays(m):
        return jnp.logical_and(lax.rem(m, pairs) > relay_limit, relay_on)

    def relay_out(m):
        return remote(
            rbuf.at[m], hal.at[m, relay_side], rf_send.at[m], h_recv.at[relay_side, m], relay_row, mem
        )

    def relay(m):
        @pl.when(relays(m))
        def _():
            remote(rbuf.at[m], rbuf.at[m], rf_send.at[m], rb_recv.at[m], high, mem).wait_recv()
            relay_out(m).start()

    @pl.when(has_high)
    def _():
        chalo_up().start()

        @pl.when(first)
        def _():
            far_up().start()

        obs_up().start()

    @pl.when(has_low)
    def _():
        chalo_down().start()

        @pl.when(first)
        def _():
            far_down().start()

        obs_down().start()

    @pl.loop(1, members)
    def _(m):
        load_ens(m).wait()

    def start_halos(near):
        @pl.when(odd == near)
        def _():
            @pl.loop(0, ahead_down)
            def _(m):
                send_down(m)

        @pl.when(odd != near)
        def _():
            @pl.loop(0, ahead_up)
            def _(m):
                send_up(m)

    start_halos(True)
    for m in range(FAR, DETOUR):
        send_detour(m)

    level = lax.broadcasted_iota(jnp.int32, (levels, width), 0)
    cell = lax.broadcasted_iota(jnp.int32, (levels, width), 1)

    def set_coef(i, a0, a1, a2):
        coef[i, 0] = 1.0 - 6.0 * DIFFUSION - jnp.abs(a0) - jnp.abs(a1) - jnp.abs(a2)
        coef[i, 1] = DIFFUSION + jnp.maximum(a0, 0.0)
        coef[i, 2] = DIFFUSION - jnp.minimum(a0, 0.0)
        coef[i, 3] = jnp.where(cell > 0, DIFFUSION + jnp.maximum(a1, 0.0), 0.0)
        coef[i, 4] = jnp.where(cell < width - 1, DIFFUSION - jnp.minimum(a1, 0.0), 0.0)
        coef[i, 5] = jnp.where(level > 0, DIFFUSION + jnp.maximum(a2, 0.0), 0.0)
        coef[i, 6] = jnp.where(level < levels - 1, DIFFUSION - jnp.minimum(a2, 0.0), 0.0)

    @pl.loop(0, rows)
    def _(i):
        set_coef(i + 2, cour[0, i], cour[1, i], cour[2, i])

    @pl.loop(0, members)
    def _(m):
        out[m] = jnp.zeros((rows, levels, width), f32)

    def no_halo(side):
        @pl.loop(0, members)
        def _(m):
            hal[m, side] = jnp.zeros((3, levels, width), f32)

    @pl.when(jnp.logical_not(has_low))
    def _():
        no_halo(0)
        coef[pl.ds(0, 2)] = jnp.zeros((2, 7, levels, width), f32)
        cext[0] = jnp.zeros((levels, width), f32)
        obsv[1] = jnp.full((2, TILE, LANES), -1, jnp.int32)
        prec[0] = jnp.zeros((groups, members, LANES), f32)

    @pl.when(jnp.logical_not(has_high))
    def _():
        no_halo(1)
        coef[pl.ds(rows + 2, 2)] = jnp.zeros((2, 7, levels, width), f32)
        cext[1] = jnp.zeros((levels, width), f32)
        obsv[2] = jnp.full((2, TILE, LANES), -1, jnp.int32)
        prec[1] = jnp.zeros((groups, members, LANES), f32)

    def edge(side, present, begin):
        @pl.when(present)
        def _():
            (chalo_down if side else chalo_up)().wait_recv()
            chalo_pass(side).start()
            (obs_down if side else obs_up)().wait_recv()

            @pl.when(first)
            def _():
                (far_down if side else far_up)().wait_recv()
                far_pass(side).start()

            @pl.when(jnp.logical_not(first))
            def _():
                far_pass(side).wait_recv()

            chalo_pass(side).wait_recv()

            @pl.loop(0, 2)
            def _(i):
                set_coef(begin + i, chalo[side, i, 0], chalo[side, i, 1], chalo[side, i, 2])

            a0 = chalo3[side]
            cext[side] = DIFFUSION + (jnp.maximum(a0, 0.0) if side else -jnp.minimum(a0, 0.0))

    @pl.when(odd)
    def _():
        edge(0, has_low, 0)

    @pl.when(jnp.logical_not(odd))
    def _():
        edge(1, has_high, rows + 2)

    start_halos(False)

    @pl.when(odd)
    def _():
        edge(1, has_high, rows + 2)

    @pl.when(jnp.logical_not(odd))
    def _():
        edge(0, has_low, 0)

    def set_hot(k):
        hit = lax.broadcasted_iota(jnp.int32, (width, LANES), 0) == obsv[k, 1, :1]
        hit = jnp.where(hit, 1.0, 0.0).astype(jnp.bfloat16)
        hot[k, :width] = hit
        hot[k, width:] = hit

    def update(c, mid, below, above):
        value = coef[c, 0] * mid
        if below is not None:
            value = value + coef[c, 1] * below
        if above is not None:
            value = value + coef[c, 2] * above
        return (
            value
            + coef[c, 3] * pltpu.roll(mid, 1, 1)
            + coef[c, 4] * pltpu.roll(mid, width - 1, 1)
            + coef[c, 5] * pltpu.roll(mid, 1, 0)
            + coef[c, 6] * pltpu.roll(mid, levels - 1, 0)
        )

    def other(d):
        return lax.rem(chip + d, chips) * 2 + core

    half = rows // 2

    def slot(src, m, h):
        return fc.at[src * members + m, pl.ds(h * half, half)]

    def send_x(d, m, h):
        at = slot(mem, m, h)
        return remote(at, at, x_send.at[d, m, h], f_recv.at[mem, m, h], row, other(d))

    def send_p(d, m, h):
        src = lax.rem(chip + d, chips) * 2 + core
        at = slot(src, m, h)
        return remote(at, at, p_send.at[d, m, h], f_recv.at[src, m, h], row, partner)

    def arrived(src, m, h):
        at = slot(src, m, h)
        return remote(at, at, p_send.at[0, 0, 0], f_recv.at[src, m, h], row, partner)

    def forward(m, h):
        for d in range(1, chips):
            arrived(other(d), m, h).wait_recv()
            send_p(d, m, h).start()

    def give(m, h):
        @pl.when(m > 0)
        def _():
            for d in range(1, chips):
                send_x(d, m - 1, h).wait_send()

        for d in range(1, chips):
            send_x(d, m, h).start()
        send_p(0, m, h).start()

        @pl.when(m >= LAG)
        def _():
            forward(m - LAG, h)

    def service(m, between):
        def source(i):
            if i < 3:
                return hal[m, 0, i]
            return ens[m, i - 3] if i < rows + 3 else hal[m, 1, i - rows - 3]

        def steps(one, two, three):
            for i in one:
                w1[i] = update(i, source(i + 1), source(i), source(i + 2))
            for i in two:
                w2[i] = update(i + 1, w1[i + 1], w1[i], w1[i + 2])
            for i in three:
                fc[mem * members + m, i] = update(i + 2, w2[i + 1], w2[i], w2[i + 2])

        @pl.when(has_low)
        def _():
            halo_up(m).wait_recv()

        @pl.when(m + ahead_up < members)
        def _():
            send_up(m + ahead_up)

        steps(range(half + 4), range(half + 2), range(half))
        give(m, 0)
        between()

        @pl.when(has_high)
        def _():
            halo_down(m).wait_recv()

        @pl.when(m + ahead_down < members)
        def _():
            send_down(m + ahead_down)

        steps(range(half + 4, rows + 4), range(half + 2, rows + 2), range(half, rows))
        give(m, 1)

        @pl.when(m + DETOUR < members)
        def _():
            send_detour(m + DETOUR)

        @pl.when(m == 0)
        def _():
            for n in range(FAR, RELAY):
                relay(n)

        @pl.when(m + RELAY < members)
        def _():
            relay(m + RELAY)

    per_pass = PER_PASS if members % PER_PASS == 0 else 1
    passes = members // per_pass

    inside = lax.broadcasted_iota(jnp.int32, (levels, LANES), 0)
    owner = lax.broadcasted_iota(jnp.int32, (levels, LANES), 1) // nobs
    pick = lax.rem(inside, TILE) == owner

    def fold(x):
        return jnp.sum(jnp.where(pick, x, 0.0).reshape(groups, TILE, LANES), axis=1)

    def profile(m, n):
        def raw(r):
            return ens[m, r] if 0 <= r < rows else None

        def first_step(r):
            return z1[r + 1] if -1 <= r <= rows else None

        def second_step(r):
            return z2[r + 2] if -2 <= r <= rows + 1 else None

        z1[0] = coef[1, 2] * raw(0)
        z1[rows + 1] = coef[rows + 2, 1] * raw(rows - 1)
        for r in range(rows):
            z1[r + 1] = update(r + 2, raw(r), raw(r - 1), raw(r + 1))
        z2[0] = coef[0, 2] * first_step(-1)
        z2[rows + 3] = coef[rows + 3, 1] * first_step(rows)
        for r in range(-1, rows + 1):
            z2[r + 2] = update(r + 2, first_step(r), first_step(r - 1), first_step(r + 1))

        def split(r, x):
            high_part = x.astype(jnp.bfloat16)
            zb[n, r + 3, :, :width] = high_part
            zb[n, r + 3, :, width:] = (x - high_part.astype(f32)).astype(jnp.bfloat16)

        split(-3, cext[0] * second_step(-2))
        split(rows + 2, cext[1] * second_step(rows + 1))
        for r in range(-2, rows + 2):
            split(r, update(r + 2, second_step(r), second_step(r - 1), second_step(r + 1)))

    def extract(begin_m):
        for k, begin, count in ((0, 3, rows), (1, 0, 3), (2, rows + 3, 3)):
            x = zb[:, pl.ds(begin, count)].reshape(per_pass * count * levels, 2 * width)
            got = jnp.dot(x, hot[k], preferred_element_type=f32)
            at = obsv[k, 0, :1] - row * rows + 3
            for n in range(per_pass):
                acc = jnp.zeros((levels, LANES), f32)
                for i in range(count):
                    base = (n * count + i) * levels
                    acc = acc + jnp.where(at == begin + i, got[base:base + levels], 0.0)
                pp[k, :, pl.ds(begin_m + n, 1)] = fold(acc)[:, None]

    def dot(a, b):
        return jnp.dot(a, b, precision=HIGHEST, preferred_element_type=f32)

    mine = pl.ds(pl.multiple_of(mem * members, members), members)

    share = total // 2

    def part_of(c):
        return pl.ds(pl.multiple_of(c * share, share), share)

    def give_low():
        return remote(pp.at[1], prec.at[1], r_send.at[1], r_recv.at[1], low, mem)

    def give_high():
        return remote(pp.at[2], prec.at[0], r_send.at[0], r_recv.at[0], high, mem)

    def stage_a():
        @pl.when(has_high)
        def _():
            give_high().start()

        @pl.when(has_low)
        def _():
            give_low().start()

    def give_prof(d):
        block = prof.at[:, mine]
        return remote(block, block, q_send.at[d], q_recv.at[mem], row, lax.rem(mem + d, mem_n))

    def stage_b():
        @pl.when(has_low)
        def _():
            give_high().wait_recv()

        @pl.when(has_high)
        def _():
            give_low().wait_recv()

        prof[:, mine] = pp[0] + prec[0] + prec[1]
        for d in range(1, mem_n):
            give_prof(d).start()

    def flat(ref):
        repeat = lax.broadcasted_iota(jnp.int32, (nobs, LANES), 1) % nobs
        repeat = jnp.where(repeat == lax.broadcasted_iota(jnp.int32, (nobs, LANES), 0), 1.0, 0.0).astype(f32)
        got = fold(dot(ref[...].T, repeat))
        return jnp.concatenate([got[q:q + 1] for q in range(groups)], axis=1)

    def give_gram(d):
        return remote(grec.at[row], grec.at[row], g_send.at[d], g_recv.at[row], lax.rem(row + d, rows_n), mem)

    def stage_c():
        for d in range(1, mem_n):
            src = lax.rem(mem + d, mem_n)
            block = prof.at[:, pl.ds(pl.multiple_of(src * members, members), members)]
            remote(block, block, q_send.at[d], q_recv.at[src], row, src).wait_recv()
        values = jnp.concatenate([prof[q] for q in range(groups)], axis=1)
        variance = flat(obs_var)
        center = jnp.mean(values, axis=0, keepdims=True)
        scaled = (values - center) / jnp.sqrt((total - 1.0) * variance)
        innovation = (flat(obs_value) - center) / jnp.sqrt(variance)
        pad = jnp.broadcast_to(innovation, (LANES - total, innovation.shape[1]))
        scal[...] = scaled
        both = jnp.concatenate([scaled, pad], axis=0)
        grec[row] = lax.dot_general(
            scal[part_of(core)], both, (((1,), (1,)), ((), ())), precision=HIGHEST, preferred_element_type=f32
        )
        for d in range(1, rows_n):
            give_gram(d).start()

    def give_sum():
        block = gall.at[part_of(core)]
        return remote(block, block, a_send.at[0], a_recv.at[core], row, partner)

    def stage_d():
        for d in range(1, rows_n):
            src = lax.rem(row + d, rows_n)
            remote(grec.at[src], grec.at[src], g_send.at[d], g_recv.at[src], src, mem).wait_recv()
        part = grec[0]
        for r in range(1, rows_n):
            part = part + grec[r]
        gall[part_of(core)] = part
        give_sum().start()

    def stage_e():
        block = gall.at[part_of(1 - core)]
        remote(block, block, a_send.at[0], a_recv.at[1 - core], row, partner).wait_recv()
        gsum = gall[...]
        ri = lax.broadcasted_iota(jnp.int32, (total, total), 0)
        ci = lax.broadcasted_iota(jnp.int32, (total, total), 1)
        eye = jnp.where(ri == ci, 1.0, 0.0).astype(f32)
        system = eye + gsum[:, :total]
        frob = jnp.sqrt(jnp.sum(jnp.sum(system * system, axis=1, keepdims=True), axis=0, keepdims=True))
        y = system / frob
        z = eye
        for it in range(NS_ITERS):
            factor = 0.5 * (3.0 * eye - (y if it == 0 else dot(z, y)))
            if it < NS_ITERS - 1:
                y = dot(y, factor)
            z = factor if it == 0 else dot(factor, z)
        root = z / jnp.sqrt(frob)
        shift = dot(root, dot(root, gsum))[:, total:total + 1] / jnp.sqrt(f32(total - 1.0))
        mixed = shift + root
        weights = 1.0 / total + mixed - jnp.mean(mixed, axis=0, keepdims=True)
        wts[...] = weights.T
        own = wts[mine].T
        for k in range(members):
            wsp[k] = jnp.broadcast_to(own[:, k:k + 1], (total, LANES))

    block = min(4, members)
    tiles = width // LANES

    def mix(m, h):
        for d in range(chips):
            arrived(lax.rem(chip + d, chips) * 2 + 1 - core, m, h).wait_recv()

        @pl.loop(0, members // block)
        def _(b):
            ws = [
                [
                    jnp.broadcast_to(wsp[b * block + k, pl.ds(s * members + m, 1)], (TILE, LANES))
                    for s in range(mem_n)
                ]
                for k in range(block)
            ]

            @pl.loop(0, half)
            def _(n):
                i = h * half + n
                for t in range(groups):
                    for c in range(tiles):
                        at = (i, pl.ds(t * TILE, TILE), pl.ds(c * LANES, LANES))
                        f = [fc[(s * members + m,) + at] for s in range(mem_n)]
                        for k in range(block):
                            acc = out[(b * block + k,) + at]
                            for s in range(mem_n):
                                acc = acc + ws[k][s] * f[s]
                            out[(b * block + k,) + at] = acc

    at_a = passes - 1
    at_b, at_c, at_d, at_e = (min(at_a + n, members - 1) for n in STAGES)

    def profiles(group, begin, end):
        @pl.when(group < passes)
        def _():
            @pl.loop(begin, end)
            def _(n):
                profile(group * per_pass + n, n)

            if end == per_pass:
                extract(group * per_pass)

    for k in range(3):
        set_hot(k)

    @pl.loop(0, members)
    def _(m):
        service(m, lambda: profiles(m, 0, per_pass // 2))
        profiles(m, per_pass // 2, per_pass)

        for at, stage in ((at_a, stage_a), (at_b, stage_b), (at_c, stage_c), (at_d, stage_d), (at_e, stage_e)):
            pl.when(m == at)(stage)

        @pl.when(m > at_e)
        def _():
            begin = jnp.minimum(m - LAG, (m - at_e - 1) * PER_MIX)
            end = jnp.minimum(m - LAG + 1, (m - at_e) * PER_MIX)

            @pl.loop(2 * begin, 2 * end)
            def _(n):
                mix(n // 2, n % 2)

    mixed_in_loop = max(0, min(members - LAG, (members - 1 - at_e) * PER_MIX))
    late = members - LAG

    @pl.loop(2 * mixed_in_loop, 2 * late)
    def _(n):
        mix(n // 2, n % 2)

    @pl.when(has_high)
    def _():
        chalo_up().wait_send()
        chalo_pass(1).wait_send()
        obs_up().wait_send()
        give_high().wait_send()

        @pl.when(first)
        def _():
            far_up().wait_send()
            far_pass(1).wait_send()

    @pl.when(has_low)
    def _():
        chalo_down().wait_send()
        chalo_pass(0).wait_send()
        obs_down().wait_send()
        give_low().wait_send()

        @pl.when(first)
        def _():
            far_down().wait_send()
            far_pass(0).wait_send()

    @pl.loop(0, members)
    def _(m):
        @pl.when(has_high)
        def _():
            halo_up(m).wait_send()

        @pl.when(has_low)
        def _():
            halo_down(m).wait_send()

        @pl.when(relays(m))
        def _():
            relay_out(m).wait_send()

        for h in range(2):
            send_p(0, m, h).wait_send()

            @pl.when(m < late)
            def _():
                for d in range(1, chips):
                    send_p(d, m, h).wait_send()

    for d in range(1, mem_n):
        give_prof(d).wait_send()
    give_sum().wait_send()
    for d in range(1, rows_n):
        give_gram(d).wait_send()

    @pl.loop(2 * late, 2 * members)
    def _(n):
        forward(n // 2, n % 2)

        @pl.when(n > 2 * late)
        def _():
            mix((n - 1) // 2, (n - 1) % 2)

    mix(members - 1, 1)

    @pl.loop(0, LAG)
    def _(n):
        for h in range(2):
            for d in range(1, chips):
                send_p(d, late + n, h).wait_send()

    for h in range(2):
        for d in range(1, chips):
            send_x(d, members - 1, h).wait_send()


def per_device(rows_n, mem_n, ensemble, courant, obs_column, obs_value, obs_var):
    members, levels, rows, width = ensemble.shape
    nobs = obs_column.shape[0]
    chips = mem_n // 2
    groups = levels // TILE
    f32 = jnp.float32
    vmem = pl.BlockSpec(memory_space=pltpu.VMEM)
    smem = pl.BlockSpec(memory_space=pltpu.SMEM)
    hbm = pl.BlockSpec(memory_space=pl.ANY)
    dma = pltpu.SemaphoreType.DMA
    total = members * mem_n
    plane = (levels, width)
    result = pl.pallas_call(
        functools.partial(kernel, rows_n, mem_n),
        out_shape=pltpu.VMEM((members, rows) + plane, f32),
        in_specs=[hbm, hbm, smem, vmem, vmem],
        out_specs=vmem,
        scratch_shapes=[
            pltpu.VMEM((members, rows) + plane, f32),
            pltpu.VMEM((3, rows) + plane, f32),
            pltpu.VMEM((2, 2, 3) + plane, f32),
            pltpu.VMEM((2,) + plane, f32),
            pltpu.VMEM((members, 2, 3) + plane, f32),
            pltpu.VMEM((rows + 4, 7) + plane, f32),
            pltpu.VMEM((2,) + plane, f32),
            pltpu.VMEM((rows + 4,) + plane, f32),
            pltpu.VMEM((rows + 2,) + plane, f32),
            pltpu.VMEM((rows + 2,) + plane, f32),
            pltpu.VMEM((rows + 4,) + plane, f32),
            pltpu.VMEM((PER_PASS, rows + 6, levels, 2 * width), jnp.bfloat16),
            pltpu.VMEM((members, 3) + plane, f32),
            pltpu.VMEM((total, rows) + plane, f32),
            pltpu.VMEM((3, 2, TILE, LANES), jnp.int32),
            pltpu.VMEM((3, 2 * width, LANES), jnp.bfloat16),
            pltpu.VMEM((3, groups, members, LANES), f32),
            pltpu.VMEM((2, groups, members, LANES), f32),
            pltpu.VMEM((groups, total, LANES), f32),
            pltpu.VMEM((total, groups * LANES), f32),
            pltpu.VMEM((rows_n, total // 2, LANES), f32),
            pltpu.VMEM((total, LANES), f32),
            pltpu.VMEM((total, total), f32),
            pltpu.VMEM((members, total, LANES), f32),
            dma((members,)), dma((1,)),
            dma((2,)), dma((2,)), dma((2,)), dma((2,)),
            dma((2,)), dma((2,)), dma((2,)), dma((2,)), dma((2,)), dma((2,)),
            dma((2, members)), dma((2, members)), dma((members,)), dma((members,)),
            dma((chips, members, 2)), dma((chips, members, 2)), dma((mem_n, members, 2)),
            dma((2,)), dma((2,)),
            dma((mem_n,)), dma((mem_n,)),
            dma((rows_n,)), dma((rows_n,)),
            dma((1,)), dma((2,)),
        ],
        compiler_params=pltpu.CompilerParams(
            collective_id=0, has_side_effects=True, vmem_limit_bytes=52 * 1024 * 1024
        ),
    )(
        ensemble.transpose(0, 2, 1, 3),
        courant.transpose(0, 2, 1, 3),
        obs_column,
        obs_value.T,
        obs_var.T,
    )
    return result.transpose(0, 2, 1, 3)


def solution(mesh):
    return jax.shard_map(
        functools.partial(per_device, mesh.shape["rows"], mesh.shape["mem"]),
        mesh=mesh,
        in_specs=(
            P("mem", None, "rows", None),
            P(None, None, "rows", None),
            P("rows"),
            P(None, "rows"),
            P(None, "rows"),
        ),
        out_specs=P("mem", None, "rows", None),
        check_vma=False,
    )
```

```python
import functools

import jax
import jax.numpy as jnp
from jax import lax
from jax.experimental import pallas as pl
from jax.experimental.pallas import tpu as pltpu
from jax.sharding import PartitionSpec as P

NS_ITERS = 4
DIFFUSION = 0.05
NEAR = 2
FAR = 1
DETOUR = 3
RELAY = 1
LAG = 2
PER_PASS = 4
STAGES = (2, 4, 6, 6)
PER_MIX = 3
LANES = 128
TILE = 8
MESH = pl.DeviceIdType.MESH
HIGHEST = lax.Precision.HIGHEST


def kernel(
    rows_n, mem_n,
    ens_any, cour_any, obs, obs_value, obs_var,
    out,
    ens, cour, chalo, chalo3, hal, coef, cext, w1, w2, z1, z2, zb, rbuf, fc,
    obsv, hot, pp, prec, prof, scal, grec, gall, wts, wsp,
    e_load, c_load,
    c_send, c_recv, cf_send, cf_recv, d_send, d_recv, df_send, df_recv, o_send, o_recv,
    h_send, h_recv, rb_recv, rf_send,
    x_send, x_recv, p_send, p_recv, r_send, r_recv, q_send, q_recv, g_send, g_recv, a_send, a_recv,
):
    members, rows, levels, width = ens.shape
    total = members * mem_n
    nobs = obs.shape[0]
    chips = mem_n // 2
    groups = levels // TILE
    row = lax.axis_index("rows")
    mem = lax.axis_index("mem")
    core = lax.rem(mem, 2)
    chip = mem // 2
    partner = chip * 2 + 1 - core
    f32 = jnp.float32

    def remote(src, dst, ssem, rsem, r, m):
        return pltpu.make_async_remote_copy(
            src_ref=src, dst_ref=dst, send_sem=ssem, recv_sem=rsem,
            device_id=(r, m), device_id_type=MESH,
        )

    def load_cour():
        return pltpu.make_async_copy(cour_any, cour, c_load.at[0])

    def load_first():
        return pltpu.make_async_copy(ens_any.at[0], ens.at[0], e_load.at[0])

    def load_rest():
        rest = pl.ds(1, members - 1)
        return pltpu.make_async_copy(ens_any.at[rest], ens.at[rest], e_load.at[1])

    load_cour().start()
    load_first().start()
    load_rest().start()

    barrier = pltpu.get_barrier_semaphore()
    for d in range(1, mem_n):
        pl.semaphore_signal(barrier, inc=1, device_id=(row, lax.rem(mem + d, mem_n)), device_id_type=MESH)
    for d in range(1, rows_n):
        pl.semaphore_signal(barrier, inc=1, device_id=(lax.rem(row + d, rows_n), mem), device_id_type=MESH)

    has_low = row > 0
    has_high = row < rows_n - 1
    low = jnp.maximum(row - 1, 0)
    high = jnp.minimum(row + 1, rows_n - 1)

    lane = lax.broadcasted_iota(jnp.int32, (TILE, LANES), 1)
    slot = lax.rem(lane, nobs)
    ox = jnp.zeros((TILE, LANES), jnp.int32)
    oy = jnp.zeros((TILE, LANES), jnp.int32)
    for p in range(nobs):
        gx = lax.div(obs[p], width)
        ox = jnp.where(slot == p, gx, ox)
        oy = jnp.where(slot == p, obs[p] - gx * width, oy)
    obsv[0, 0] = ox
    obsv[0, 1] = oy

    load_cour().wait()
    load_first().wait()
    pl.semaphore_wait(barrier, mem_n - 1 + rows_n - 1)

    def chalo_up():
        return remote(cour.at[:, rows - 2 + core], chalo.at[0, core], c_send.at[0], c_recv.at[0], high, mem)

    def chalo_down():
        return remote(cour.at[:, core], chalo.at[1, core], c_send.at[1], c_recv.at[1], low, mem)

    def chalo_pass(side):
        return remote(chalo.at[side, core], chalo.at[side, core], cf_send.at[side], cf_recv.at[side], row, partner)

    def far_up():
        return remote(cour.at[0, rows - 3], chalo3.at[0], d_send.at[0], d_recv.at[0], high, mem)

    def far_down():
        return remote(cour.at[0, 2], chalo3.at[1], d_send.at[1], d_recv.at[1], low, mem)

    def far_pass(side):
        return remote(chalo3.at[side], chalo3.at[side], df_send.at[side], df_recv.at[side], row, partner)

    def obs_up():
        return remote(obsv.at[0], obsv.at[1], o_send.at[0], o_recv.at[0], high, mem)

    def obs_down():
        return remote(obsv.at[0], obsv.at[2], o_send.at[1], o_recv.at[1], low, mem)

    def halo_up(m):
        return remote(ens.at[m, pl.ds(rows - 3, 3)], hal.at[m, 0], h_send.at[0], h_recv.at[0, m], high, mem)

    def halo_down(m):
        return remote(ens.at[m, pl.ds(0, 3)], hal.at[m, 1], h_send.at[1], h_recv.at[1, m], low, mem)

    first = core == 0

    odd = lax.rem(row, 2) == 1
    ahead_up = jnp.where(odd, FAR, NEAR)
    ahead_down = jnp.where(odd, NEAR, FAR)

    pairs = max(1, rows_n // 2)
    pair = row // 2
    send_limit = jnp.where(odd, pair, pairs - 1 - pair)
    relay_limit = jnp.where(odd, pairs - 1 - pair, pair)
    relay_side = jnp.where(odd, 1, 0)
    relay_on = jnp.logical_and(jnp.where(odd, row - 2, row) >= 0, jnp.where(odd, row, row + 2) < rows_n)
    relay_row = jnp.clip(jnp.where(odd, row - 2, row + 2), 0, rows_n - 1)

    def detour(m):
        return jnp.logical_and(lax.rem(m, pairs) > send_limit, jnp.logical_and(has_low, has_high))

    def send_up(m):
        @pl.when(jnp.logical_and(has_high, jnp.logical_not(jnp.logical_and(odd, detour(m)))))
        def _():
            halo_up(m).start()

    def send_down(m):
        @pl.when(jnp.logical_and(has_low, jnp.logical_or(odd, jnp.logical_not(detour(m)))))
        def _():
            halo_down(m).start()

    def send_detour(m):
        @pl.when(jnp.logical_and(odd, detour(m)))
        def _():
            remote(ens.at[m, pl.ds(rows - 3, 3)], rbuf.at[m], h_send.at[0], rb_recv.at[m], low, mem).start()

        @pl.when(jnp.logical_and(jnp.logical_not(odd), detour(m)))
        def _():
            remote(ens.at[m, pl.ds(0, 3)], rbuf.at[m], h_send.at[1], rb_recv.at[m], high, mem).start()

    def relays(m):
        return jnp.logical_and(lax.rem(m, pairs) > relay_limit, relay_on)

    def relay_out(m):
        return remote(
            rbuf.at[m], hal.at[m, relay_side], rf_send.at[m], h_recv.at[relay_side, m], relay_row, mem
        )

    def relay(m):
        @pl.when(relays(m))
        def _():
            remote(rbuf.at[m], rbuf.at[m], rf_send.at[m], rb_recv.at[m], high, mem).wait_recv()
            relay_out(m).start()

    @pl.when(has_high)
    def _():
        chalo_up().start()

        @pl.when(first)
        def _():
            far_up().start()

        obs_up().start()

    @pl.when(has_low)
    def _():
        chalo_down().start()

        @pl.when(first)
        def _():
            far_down().start()

        obs_down().start()

    load_rest().wait()

    def start_halos(near):
        @pl.when(odd == near)
        def _():
            @pl.loop(0, ahead_down)
            def _(m):
                send_down(m)

        @pl.when(odd != near)
        def _():
            @pl.loop(0, ahead_up)
            def _(m):
                send_up(m)

    start_halos(True)
    for m in range(FAR, DETOUR):
        send_detour(m)

    level = lax.broadcasted_iota(jnp.int32, (levels, width), 0)
    cell = lax.broadcasted_iota(jnp.int32, (levels, width), 1)

    def set_coef(i, a0, a1, a2):
        coef[i, 0] = 1.0 - 6.0 * DIFFUSION - jnp.abs(a0) - jnp.abs(a1) - jnp.abs(a2)
        coef[i, 1] = DIFFUSION + jnp.maximum(a0, 0.0)
        coef[i, 2] = DIFFUSION - jnp.minimum(a0, 0.0)
        coef[i, 3] = jnp.where(cell > 0, DIFFUSION + jnp.maximum(a1, 0.0), 0.0)
        coef[i, 4] = jnp.where(cell < width - 1, DIFFUSION - jnp.minimum(a1, 0.0), 0.0)
        coef[i, 5] = jnp.where(level > 0, DIFFUSION + jnp.maximum(a2, 0.0), 0.0)
        coef[i, 6] = jnp.where(level < levels - 1, DIFFUSION - jnp.minimum(a2, 0.0), 0.0)

    @pl.loop(0, rows)
    def _(i):
        set_coef(i + 2, cour[0, i], cour[1, i], cour[2, i])

    @pl.loop(0, members)
    def _(m):
        out[m] = jnp.zeros((rows, levels, width), f32)

    def no_halo(side):
        @pl.loop(0, members)
        def _(m):
            hal[m, side] = jnp.zeros((3, levels, width), f32)

    @pl.when(jnp.logical_not(has_low))
    def _():
        no_halo(0)
        coef[pl.ds(0, 2)] = jnp.zeros((2, 7, levels, width), f32)
        cext[0] = jnp.zeros((levels, width), f32)
        obsv[1] = jnp.full((2, TILE, LANES), -1, jnp.int32)
        prec[0] = jnp.zeros((groups, members, LANES), f32)

    @pl.when(jnp.logical_not(has_high))
    def _():
        no_halo(1)
        coef[pl.ds(rows + 2, 2)] = jnp.zeros((2, 7, levels, width), f32)
        cext[1] = jnp.zeros((levels, width), f32)
        obsv[2] = jnp.full((2, TILE, LANES), -1, jnp.int32)
        prec[1] = jnp.zeros((groups, members, LANES), f32)

    def edge(side, present, begin):
        @pl.when(present)
        def _():
            (chalo_down if side else chalo_up)().wait_recv()
            chalo_pass(side).start()
            (obs_down if side else obs_up)().wait_recv()

            @pl.when(first)
            def _():
                (far_down if side else far_up)().wait_recv()
                far_pass(side).start()

            @pl.when(jnp.logical_not(first))
            def _():
                far_pass(side).wait_recv()

            chalo_pass(side).wait_recv()

            @pl.loop(0, 2)
            def _(i):
                set_coef(begin + i, chalo[side, i, 0], chalo[side, i, 1], chalo[side, i, 2])

            a0 = chalo3[side]
            cext[side] = DIFFUSION + (jnp.maximum(a0, 0.0) if side else -jnp.minimum(a0, 0.0))

    @pl.when(odd)
    def _():
        edge(0, has_low, 0)

    @pl.when(jnp.logical_not(odd))
    def _():
        edge(1, has_high, rows + 2)

    start_halos(False)

    @pl.when(odd)
    def _():
        edge(1, has_high, rows + 2)

    @pl.when(jnp.logical_not(odd))
    def _():
        edge(0, has_low, 0)

    def set_hot(k):
        hit = lax.broadcasted_iota(jnp.int32, (width, LANES), 0) == obsv[k, 1, :1]
        hit = jnp.where(hit, 1.0, 0.0).astype(jnp.bfloat16)
        hot[k, :width] = hit
        hot[k, width:] = hit

    def update(c, mid, below, above):
        value = coef[c, 0] * mid
        if below is not None:
            value = value + coef[c, 1] * below
        if above is not None:
            value = value + coef[c, 2] * above
        return (
            value
            + coef[c, 3] * pltpu.roll(mid, 1, 1)
            + coef[c, 4] * pltpu.roll(mid, width - 1, 1)
            + coef[c, 5] * pltpu.roll(mid, 1, 0)
            + coef[c, 6] * pltpu.roll(mid, levels - 1, 0)
        )

    def other(d):
        return lax.rem(chip + d, chips) * 2 + core

    half = rows // 2

    def slot(src, m, h):
        return fc.at[src * members + m, pl.ds(h * half, half)]

    late = members - LAG

    def send_x(d, m, h):
        at = slot(mem, m, h)
        return remote(at, at, x_send.at[d - 1, h], x_recv.at[chips - d - 1, m, h], row, other(d))

    def from_x(d, m, h):
        at = slot(other(d), m, h)
        return remote(at, at, x_send.at[0, 0], x_recv.at[d - 1, m, h], row, other(d))

    def piece(d, m, h):
        return jnp.where(m < late, m, late + ((m - late) * chips + d) * 2 + h)

    def send_p(d, m, h):
        src = lax.rem(chip + d, chips) * 2 + core
        at = slot(src, m, h)
        return remote(at, at, p_send.at[min(d, 1)], p_recv.at[piece(d, m, h)], row, partner)

    def from_p(d, m, h):
        at = slot(lax.rem(chip + d, chips) * 2 + 1 - core, m, h)
        return remote(at, at, p_send.at[0], p_recv.at[piece(d, m, h)], row, partner)

    def from_p_whole(m):
        at = fc.at[pl.ds(0, chips)]
        return remote(at, at, p_send.at[0], p_recv.at[m], row, partner)

    def forward(m, h):
        for d in range(1, chips):
            from_x(d, m, h).wait_recv()
            send_p(d, m, h).start()

    def give(m, h):
        @pl.when(m > 0)
        def _():
            for d in range(1, chips):
                send_x(d, m - 1, h).wait_send()

        for d in range(1, chips):
            send_x(d, m, h).start()
        send_p(0, m, h).start()

        @pl.when(m >= LAG)
        def _():
            forward(m - LAG, h)

    def service(m, between):
        def source(i):
            if i < 3:
                return hal[m, 0, i]
            return ens[m, i - 3] if i < rows + 3 else hal[m, 1, i - rows - 3]

        def steps(one, two, three):
            for i in one:
                w1[i] = update(i, source(i + 1), source(i), source(i + 2))
            for i in two:
                w2[i] = update(i + 1, w1[i + 1], w1[i], w1[i + 2])
            for i in three:
                fc[mem * members + m, i] = update(i + 2, w2[i + 1], w2[i], w2[i + 2])

        @pl.when(has_low)
        def _():
            halo_up(m).wait_recv()

        @pl.when(m + ahead_up < members)
        def _():
            send_up(m + ahead_up)

        steps(range(half + 4), range(half + 2), range(half))
        give(m, 0)
        between()

        @pl.when(has_high)
        def _():
            halo_down(m).wait_recv()

        @pl.when(m + ahead_down < members)
        def _():
            send_down(m + ahead_down)

        steps(range(half + 4, rows + 4), range(half + 2, rows + 2), range(half, rows))
        give(m, 1)

        @pl.when(m + DETOUR < members)
        def _():
            send_detour(m + DETOUR)

        @pl.when(m == 0)
        def _():
            for n in range(FAR, RELAY):
                relay(n)

        @pl.when(m + RELAY < members)
        def _():
            relay(m + RELAY)

    per_pass = PER_PASS if members % PER_PASS == 0 else 1
    passes = members // per_pass

    inside = lax.broadcasted_iota(jnp.int32, (levels, LANES), 0)
    owner = lax.broadcasted_iota(jnp.int32, (levels, LANES), 1) // nobs
    pick = lax.rem(inside, TILE) == owner

    def fold(x):
        return jnp.sum(jnp.where(pick, x, 0.0).reshape(groups, TILE, LANES), axis=1)

    def profile(m, n):
        def raw(r):
            return ens[m, r] if 0 <= r < rows else None

        def first_step(r):
            return z1[r + 1] if -1 <= r <= rows else None

        def second_step(r):
            return z2[r + 2] if -2 <= r <= rows + 1 else None

        z1[0] = coef[1, 2] * raw(0)
        z1[rows + 1] = coef[rows + 2, 1] * raw(rows - 1)
        for r in range(rows):
            z1[r + 1] = update(r + 2, raw(r), raw(r - 1), raw(r + 1))
        z2[0] = coef[0, 2] * first_step(-1)
        z2[rows + 3] = coef[rows + 3, 1] * first_step(rows)
        for r in range(-1, rows + 1):
            z2[r + 2] = update(r + 2, first_step(r), first_step(r - 1), first_step(r + 1))

        def split(r, x):
            high_part = x.astype(jnp.bfloat16)
            zb[n, r + 3, :, :width] = high_part
            zb[n, r + 3, :, width:] = (x - high_part.astype(f32)).astype(jnp.bfloat16)

        split(-3, cext[0] * second_step(-2))
        split(rows + 2, cext[1] * second_step(rows + 1))
        for r in range(-2, rows + 2):
            split(r, update(r + 2, second_step(r), second_step(r - 1), second_step(r + 1)))

    def extract(begin_m):
        for k, begin, count in ((0, 3, rows), (1, 0, 3), (2, rows + 3, 3)):
            x = zb[:, pl.ds(begin, count)].reshape(per_pass * count * levels, 2 * width)
            got = jnp.dot(x, hot[k], preferred_element_type=f32)
            at = obsv[k, 0, :1] - row * rows + 3
            for n in range(per_pass):
                acc = jnp.zeros((levels, LANES), f32)
                for i in range(count):
                    base = (n * count + i) * levels
                    acc = acc + jnp.where(at == begin + i, got[base:base + levels], 0.0)
                pp[k, :, pl.ds(begin_m + n, 1)] = fold(acc)[:, None]

    def dot(a, b):
        return jnp.dot(a, b, precision=HIGHEST, preferred_element_type=f32)

    mine = pl.ds(pl.multiple_of(mem * members, members), members)

    share = total // 2

    def part_of(c):
        return pl.ds(pl.multiple_of(c * share, share), share)

    def give_low():
        return remote(pp.at[1], prec.at[1], r_send.at[1], r_recv.at[1], low, mem)

    def give_high():
        return remote(pp.at[2], prec.at[0], r_send.at[0], r_recv.at[0], high, mem)

    def stage_a():
        @pl.when(has_high)
        def _():
            give_high().start()

        @pl.when(has_low)
        def _():
            give_low().start()

    def give_prof(d):
        block = prof.at[:, mine]
        return remote(block, block, q_send.at[0], q_recv.at[0], row, lax.rem(mem + d, mem_n))

    def all_profiles():
        block = prof.at[:, pl.ds(0, (mem_n - 1) * members)]
        return remote(block, block, q_send.at[0], q_recv.at[0], row, partner)

    def stage_b():
        @pl.when(has_low)
        def _():
            give_high().wait_recv()

        @pl.when(has_high)
        def _():
            give_low().wait_recv()

        prof[:, mine] = pp[0] + prec[0] + prec[1]
        for d in range(1, mem_n):
            give_prof(d).start()

    def flat(ref):
        repeat = lax.broadcasted_iota(jnp.int32, (nobs, LANES), 1) % nobs
        repeat = jnp.where(repeat == lax.broadcasted_iota(jnp.int32, (nobs, LANES), 0), 1.0, 0.0).astype(f32)
        got = fold(dot(ref[...].T, repeat))
        return jnp.concatenate([got[q:q + 1] for q in range(groups)], axis=1)

    def give_gram(d):
        return remote(grec.at[row], grec.at[row], g_send.at[0], g_recv.at[0], lax.rem(row + d, rows_n), mem)

    def all_grams():
        block = grec.at[pl.ds(0, rows_n - 1)]
        return remote(block, block, g_send.at[0], g_recv.at[0], lax.rem(row + 1, rows_n), mem)

    def stage_c():
        all_profiles().wait_recv()
        values = jnp.concatenate([prof[q] for q in range(groups)], axis=1)
        variance = flat(obs_var)
        center = jnp.mean(values, axis=0, keepdims=True)
        scaled = (values - center) / jnp.sqrt((total - 1.0) * variance)
        innovation = (flat(obs_value) - center) / jnp.sqrt(variance)
        pad = jnp.broadcast_to(innovation, (LANES - total, innovation.shape[1]))
        scal[...] = scaled
        both = jnp.concatenate([scaled, pad], axis=0)
        grec[row] = lax.dot_general(
            scal[part_of(core)], both, (((1,), (1,)), ((), ())), precision=HIGHEST, preferred_element_type=f32
        )
        for d in range(1, rows_n):
            give_gram(d).start()

    def give_sum():
        block = gall.at[part_of(core)]
        return remote(block, block, a_send.at[0], a_recv.at[core], row, partner)

    def stage_d():
        all_grams().wait_recv()
        part = grec[0]
        for r in range(1, rows_n):
            part = part + grec[r]
        gall[part_of(core)] = part
        give_sum().start()

    def stage_e():
        block = gall.at[part_of(1 - core)]
        remote(block, block, a_send.at[0], a_recv.at[1 - core], row, partner).wait_recv()
        gsum = gall[...]
        ri = lax.broadcasted_iota(jnp.int32, (total, total), 0)
        ci = lax.broadcasted_iota(jnp.int32, (total, total), 1)
        eye = jnp.where(ri == ci, 1.0, 0.0).astype(f32)
        system = eye + gsum[:, :total]
        frob = jnp.sqrt(jnp.sum(jnp.sum(system * system, axis=1, keepdims=True), axis=0, keepdims=True))
        y = system / frob
        z = eye
        for it in range(NS_ITERS):
            factor = 0.5 * (3.0 * eye - (y if it == 0 else dot(z, y)))
            if it < NS_ITERS - 1:
                y = dot(y, factor)
            z = factor if it == 0 else dot(factor, z)
        root = z / jnp.sqrt(frob)
        shift = dot(root, dot(root, gsum))[:, total:total + 1] / jnp.sqrt(f32(total - 1.0))
        mixed = shift + root
        weights = 1.0 / total + mixed - jnp.mean(mixed, axis=0, keepdims=True)
        wts[...] = weights.T
        own = wts[mine].T
        for k in range(members):
            wsp[k] = jnp.broadcast_to(own[:, k:k + 1], (total, LANES))

    block = min(4, members)
    tiles = width // LANES

    def mix(m, h):
        @pl.when(jnp.logical_and(m < late, h == 0))
        def _():
            from_p_whole(m).wait_recv()

        @pl.when(m >= late)
        def _():
            for d in range(chips):
                from_p(d, m, h).wait_recv()

        @pl.loop(0, members // block)
        def _(b):
            ws = [
                [
                    jnp.broadcast_to(wsp[b * block + k, pl.ds(s * members + m, 1)], (TILE, LANES))
                    for s in range(mem_n)
                ]
                for k in range(block)
            ]

            @pl.loop(0, half)
            def _(n):
                i = h * half + n
                for t in range(groups):
                    for c in range(tiles):
                        at = (i, pl.ds(t * TILE, TILE), pl.ds(c * LANES, LANES))
                        f = [fc[(s * members + m,) + at] for s in range(mem_n)]
                        for k in range(block):
                            acc = out[(b * block + k,) + at]
                            for s in range(mem_n):
                                acc = acc + ws[k][s] * f[s]
                            out[(b * block + k,) + at] = acc

    at_a = passes - 1
    at_b, at_c, at_d, at_e = (min(at_a + n, members - 1) for n in STAGES)

    def profiles(group, begin, end):
        @pl.when(group < passes)
        def _():
            @pl.loop(begin, end)
            def _(n):
                profile(group * per_pass + n, n)

            if end == per_pass:
                extract(group * per_pass)

    for k in range(3):
        set_hot(k)

    @pl.loop(0, members)
    def _(m):
        service(m, lambda: profiles(m, 0, per_pass // 2))
        profiles(m, per_pass // 2, per_pass)

        for at, stage in ((at_a, stage_a), (at_b, stage_b), (at_c, stage_c), (at_d, stage_d), (at_e, stage_e)):
            pl.when(m == at)(stage)

        @pl.when(m > at_e)
        def _():
            begin = jnp.minimum(m - LAG, (m - at_e - 1) * PER_MIX)
            end = jnp.minimum(m - LAG + 1, (m - at_e) * PER_MIX)

            @pl.loop(2 * begin, 2 * end)
            def _(n):
                mix(n // 2, n % 2)

    mixed_in_loop = max(0, min(members - LAG, (members - 1 - at_e) * PER_MIX))
    @pl.loop(2 * mixed_in_loop, 2 * late)
    def _(n):
        mix(n // 2, n % 2)

    @pl.when(has_high)
    def _():
        chalo_up().wait_send()
        chalo_pass(1).wait_send()
        obs_up().wait_send()
        give_high().wait_send()
        remote(rbuf, rbuf, h_send.at[0], rb_recv.at[0], high, mem).wait_send()

        @pl.when(first)
        def _():
            far_up().wait_send()
            far_pass(1).wait_send()

    @pl.when(has_low)
    def _():
        chalo_down().wait_send()
        chalo_pass(0).wait_send()
        obs_down().wait_send()
        give_low().wait_send()
        remote(rbuf, rbuf, h_send.at[1], rb_recv.at[0], low, mem).wait_send()

        @pl.when(first)
        def _():
            far_down().wait_send()
            far_pass(0).wait_send()

    @pl.loop(0, members)
    def _(m):
        @pl.when(relays(m))
        def _():
            relay_out(m).wait_send()

    all_profiles().wait_send()
    give_sum().wait_send()
    all_grams().wait_send()

    @pl.loop(2 * late, 2 * members)
    def _(n):
        forward(n // 2, n % 2)
        mix(n // 2, n % 2)

    for h in range(2):
        for d in range(1, chips):
            send_x(d, members - 1, h).wait_send()
    for part, count in ((0, members), (1, (chips - 1) * members)):
        at = fc.at[pl.ds(0, count)]
        remote(at, at, p_send.at[part], p_recv.at[0], row, partner).wait_send()


def per_device(rows_n, mem_n, ensemble, courant, obs_column, obs_value, obs_var):
    members, levels, rows, width = ensemble.shape
    nobs = obs_column.shape[0]
    chips = mem_n // 2
    groups = levels // TILE
    f32 = jnp.float32
    vmem = pl.BlockSpec(memory_space=pltpu.VMEM)
    smem = pl.BlockSpec(memory_space=pltpu.SMEM)
    hbm = pl.BlockSpec(memory_space=pl.ANY)
    dma = pltpu.SemaphoreType.DMA
    total = members * mem_n
    plane = (levels, width)
    result = pl.pallas_call(
        functools.partial(kernel, rows_n, mem_n),
        out_shape=pltpu.VMEM((members, rows) + plane, f32),
        in_specs=[hbm, hbm, smem, vmem, vmem],
        out_specs=vmem,
        scratch_shapes=[
            pltpu.VMEM((members, rows) + plane, f32),
            pltpu.VMEM((3, rows) + plane, f32),
            pltpu.VMEM((2, 2, 3) + plane, f32),
            pltpu.VMEM((2,) + plane, f32),
            pltpu.VMEM((members, 2, 3) + plane, f32),
            pltpu.VMEM((rows + 4, 7) + plane, f32),
            pltpu.VMEM((2,) + plane, f32),
            pltpu.VMEM((rows + 4,) + plane, f32),
            pltpu.VMEM((rows + 2,) + plane, f32),
            pltpu.VMEM((rows + 2,) + plane, f32),
            pltpu.VMEM((rows + 4,) + plane, f32),
            pltpu.VMEM((PER_PASS, rows + 6, levels, 2 * width), jnp.bfloat16),
            pltpu.VMEM((members, 3) + plane, f32),
            pltpu.VMEM((total, rows) + plane, f32),
            pltpu.VMEM((3, 2, TILE, LANES), jnp.int32),
            pltpu.VMEM((3, 2 * width, LANES), jnp.bfloat16),
            pltpu.VMEM((3, groups, members, LANES), f32),
            pltpu.VMEM((2, groups, members, LANES), f32),
            pltpu.VMEM((groups, total, LANES), f32),
            pltpu.VMEM((total, groups * LANES), f32),
            pltpu.VMEM((rows_n, total // 2, LANES), f32),
            pltpu.VMEM((total, LANES), f32),
            pltpu.VMEM((total, total), f32),
            pltpu.VMEM((members, total, LANES), f32),
            dma((2,)), dma((1,)),
            dma((2,)), dma((2,)), dma((2,)), dma((2,)),
            dma((2,)), dma((2,)), dma((2,)), dma((2,)), dma((2,)), dma((2,)),
            dma((2,)), dma((2, members)), dma((members,)), dma((members,)),
            dma((chips - 1, 2)), dma((chips - 1, members, 2)), dma((2,)), dma((members - LAG + LAG * chips * 2,)),
            dma((2,)), dma((2,)),
            dma((1,)), dma((1,)),
            dma((1,)), dma((1,)),
            dma((1,)), dma((2,)),
        ],
        compiler_params=pltpu.CompilerParams(
            collective_id=0, has_side_effects=True, vmem_limit_bytes=52 * 1024 * 1024
        ),
    )(
        ensemble.transpose(0, 2, 1, 3),
        courant.transpose(0, 2, 1, 3),
        obs_column,
        obs_value.T,
        obs_var.T,
    )
    return result.transpose(0, 2, 1, 3)


def solution(mesh):
    return jax.shard_map(
        functools.partial(per_device, mesh.shape["rows"], mesh.shape["mem"]),
        mesh=mesh,
        in_specs=(
            P("mem", None, "rows", None),
            P(None, None, "rows", None),
            P("rows"),
            P(None, "rows"),
            P(None, "rows"),
        ),
        out_specs=P("mem", None, "rows", None),
        check_vma=False,
    )
```

```python
import functools

import jax
import jax.numpy as jnp
from jax import lax
from jax.experimental import pallas as pl
from jax.experimental.pallas import tpu as pltpu
from jax.sharding import PartitionSpec as P

NS_ITERS = 4
DIFFUSION = 0.05
NEAR = 2
FAR = 1
DETOUR = 3
RELAY = 1
LAG = 2
PER_PASS = 4
STAGES = (2, 4, 6, 6)
PER_MIX = 3
LANES = 128
TILE = 8
MESH = pl.DeviceIdType.MESH
HIGHEST = lax.Precision.HIGHEST


def kernel(
    rows_n, mem_n,
    ens_any, cour_any, obs, obs_value, obs_var,
    out,
    ens, cour, chalo, chalo3, hal, coef, cext, w1, w2, z1, z2, zb, rbuf, fc,
    obsv, hot, pp, prec, prof, scal, grec, gall, wts, wsp,
    e_load, c_load,
    c_send, c_recv, cf_send, cf_recv, d_send, d_recv, df_send, df_recv, o_send, o_recv,
    h_send, h_recv, rb_recv, rf_send,
    x_send, x_recv, p_send, p_recv, r_send, r_recv, q_send, q_recv, g_send, g_recv, a_send, a_recv,
):
    members, rows, levels, width = ens.shape
    total = members * mem_n
    nobs = obs.shape[0]
    chips = mem_n // 2
    groups = levels // TILE
    row = lax.axis_index("rows")
    mem = lax.axis_index("mem")
    core = lax.rem(mem, 2)
    chip = mem // 2
    partner = chip * 2 + 1 - core
    f32 = jnp.float32

    def remote(src, dst, ssem, rsem, r, m):
        return pltpu.make_async_remote_copy(
            src_ref=src, dst_ref=dst, send_sem=ssem, recv_sem=rsem,
            device_id=(r, m), device_id_type=MESH,
        )

    def load_cour():
        return pltpu.make_async_copy(cour_any, cour, c_load.at[0])

    def load_first():
        return pltpu.make_async_copy(ens_any.at[0], ens.at[0], e_load.at[0])

    def load_rest():
        rest = pl.ds(1, members - 1)
        return pltpu.make_async_copy(ens_any.at[rest], ens.at[rest], e_load.at[1])

    load_cour().start()
    load_first().start()
    load_rest().start()

    barrier = pltpu.get_barrier_semaphore()
    for d in range(1, mem_n):
        pl.semaphore_signal(barrier, inc=1, device_id=(row, lax.rem(mem + d, mem_n)), device_id_type=MESH)
    for d in range(1, rows_n):
        pl.semaphore_signal(barrier, inc=1, device_id=(lax.rem(row + d, rows_n), mem), device_id_type=MESH)

    has_low = row > 0
    has_high = row < rows_n - 1
    low = jnp.maximum(row - 1, 0)
    high = jnp.minimum(row + 1, rows_n - 1)

    lane = lax.broadcasted_iota(jnp.int32, (TILE, LANES), 1)
    slot = lax.rem(lane, nobs)
    ox = jnp.zeros((TILE, LANES), jnp.int32)
    oy = jnp.zeros((TILE, LANES), jnp.int32)
    for p in range(nobs):
        gx = lax.div(obs[p], width)
        ox = jnp.where(slot == p, gx, ox)
        oy = jnp.where(slot == p, obs[p] - gx * width, oy)
    obsv[0, 0] = ox
    obsv[0, 1] = oy

    load_cour().wait()
    load_first().wait()
    pl.semaphore_wait(barrier, mem_n - 1 + rows_n - 1)

    def chalo_up():
        return remote(cour.at[:, rows - 2 + core], chalo.at[0, core], c_send.at[0], c_recv.at[0], high, mem)

    def chalo_down():
        return remote(cour.at[:, core], chalo.at[1, core], c_send.at[1], c_recv.at[1], low, mem)

    def chalo_pass(side):
        return remote(chalo.at[side, core], chalo.at[side, core], cf_send.at[side], cf_recv.at[side], row, partner)

    def far_up():
        return remote(cour.at[0, rows - 3], chalo3.at[0], d_send.at[0], d_recv.at[0], high, mem)

    def far_down():
        return remote(cour.at[0, 2], chalo3.at[1], d_send.at[1], d_recv.at[1], low, mem)

    def far_pass(side):
        return remote(chalo3.at[side], chalo3.at[side], df_send.at[side], df_recv.at[side], row, partner)

    def obs_up():
        return remote(obsv.at[0], obsv.at[1], o_send.at[0], o_recv.at[0], high, mem)

    def obs_down():
        return remote(obsv.at[0], obsv.at[2], o_send.at[1], o_recv.at[1], low, mem)

    def halo_up(m):
        return remote(ens.at[m, pl.ds(rows - 3, 3)], hal.at[m, 0], h_send.at[0], h_recv.at[0, m], high, mem)

    def halo_down(m):
        return remote(ens.at[m, pl.ds(0, 3)], hal.at[m, 1], h_send.at[1], h_recv.at[1, m], low, mem)

    first = core == 0

    odd = lax.rem(row, 2) == 1
    ahead_up = jnp.where(odd, FAR, NEAR)
    ahead_down = jnp.where(odd, NEAR, FAR)

    pairs = max(1, rows_n // 2)
    pair = row // 2
    send_limit = jnp.where(odd, pair, pairs - 1 - pair)
    relay_limit = jnp.where(odd, pairs - 1 - pair, pair)
    relay_side = jnp.where(odd, 1, 0)
    relay_on = jnp.logical_and(jnp.where(odd, row - 2, row) >= 0, jnp.where(odd, row, row + 2) < rows_n)
    relay_row = jnp.clip(jnp.where(odd, row - 2, row + 2), 0, rows_n - 1)

    def detour(m):
        return jnp.logical_and(lax.rem(m, pairs) > send_limit, jnp.logical_and(has_low, has_high))

    def send_up(m):
        @pl.when(jnp.logical_and(has_high, jnp.logical_not(jnp.logical_and(odd, detour(m)))))
        def _():
            halo_up(m).start()

    def send_down(m):
        @pl.when(jnp.logical_and(has_low, jnp.logical_or(odd, jnp.logical_not(detour(m)))))
        def _():
            halo_down(m).start()

    def send_detour(m):
        @pl.when(jnp.logical_and(odd, detour(m)))
        def _():
            remote(ens.at[m, pl.ds(rows - 3, 3)], rbuf.at[m], h_send.at[0], rb_recv.at[m], low, mem).start()

        @pl.when(jnp.logical_and(jnp.logical_not(odd), detour(m)))
        def _():
            remote(ens.at[m, pl.ds(0, 3)], rbuf.at[m], h_send.at[1], rb_recv.at[m], high, mem).start()

    def relays(m):
        return jnp.logical_and(lax.rem(m, pairs) > relay_limit, relay_on)

    def relay_out(m):
        return remote(
            rbuf.at[m], hal.at[m, relay_side], rf_send.at[m], h_recv.at[relay_side, m], relay_row, mem
        )

    def relay(m):
        @pl.when(relays(m))
        def _():
            remote(rbuf.at[m], rbuf.at[m], rf_send.at[m], rb_recv.at[m], high, mem).wait_recv()
            relay_out(m).start()

    @pl.when(has_high)
    def _():
        chalo_up().start()

        @pl.when(first)
        def _():
            far_up().start()

        obs_up().start()

    @pl.when(has_low)
    def _():
        chalo_down().start()

        @pl.when(first)
        def _():
            far_down().start()

        obs_down().start()

    load_rest().wait()

    def start_halos(near):
        @pl.when(odd == near)
        def _():
            @pl.loop(0, ahead_down)
            def _(m):
                send_down(m)

        @pl.when(odd != near)
        def _():
            @pl.loop(0, ahead_up)
            def _(m):
                send_up(m)

    start_halos(True)
    for m in range(FAR, DETOUR):
        send_detour(m)

    level = lax.broadcasted_iota(jnp.int32, (levels, width), 0)
    cell = lax.broadcasted_iota(jnp.int32, (levels, width), 1)

    def set_coef(i, a0, a1, a2):
        coef[i, 0] = 1.0 - 6.0 * DIFFUSION - jnp.abs(a0) - jnp.abs(a1) - jnp.abs(a2)
        coef[i, 1] = DIFFUSION + jnp.maximum(a0, 0.0)
        coef[i, 2] = DIFFUSION - jnp.minimum(a0, 0.0)
        coef[i, 3] = jnp.where(cell > 0, DIFFUSION + jnp.maximum(a1, 0.0), 0.0)
        coef[i, 4] = jnp.where(cell < width - 1, DIFFUSION - jnp.minimum(a1, 0.0), 0.0)
        coef[i, 5] = jnp.where(level > 0, DIFFUSION + jnp.maximum(a2, 0.0), 0.0)
        coef[i, 6] = jnp.where(level < levels - 1, DIFFUSION - jnp.minimum(a2, 0.0), 0.0)

    @pl.loop(0, rows)
    def _(i):
        set_coef(i + 2, cour[0, i], cour[1, i], cour[2, i])

    @pl.loop(0, members)
    def _(m):
        out[m] = jnp.zeros((rows, levels, width), f32)

    def no_halo(side):
        @pl.loop(0, members)
        def _(m):
            hal[m, side] = jnp.zeros((3, levels, width), f32)

    @pl.when(jnp.logical_not(has_low))
    def _():
        no_halo(0)
        coef[pl.ds(0, 2)] = jnp.zeros((2, 7, levels, width), f32)
        cext[0] = jnp.zeros((levels, width), f32)
        obsv[1] = jnp.full((2, TILE, LANES), -1, jnp.int32)
        prec[0] = jnp.zeros((groups, members, LANES), f32)

    @pl.when(jnp.logical_not(has_high))
    def _():
        no_halo(1)
        coef[pl.ds(rows + 2, 2)] = jnp.zeros((2, 7, levels, width), f32)
        cext[1] = jnp.zeros((levels, width), f32)
        obsv[2] = jnp.full((2, TILE, LANES), -1, jnp.int32)
        prec[1] = jnp.zeros((groups, members, LANES), f32)

    def edge_in(side, present):
        @pl.when(present)
        def _():
            (chalo_down if side else chalo_up)().wait_recv()
            chalo_pass(side).start()

    def edge_more(side, present):
        @pl.when(present)
        def _():
            @pl.when(first)
            def _():
                (far_down if side else far_up)().wait_recv()
                far_pass(side).start()

            (obs_down if side else obs_up)().wait_recv()

    def edge_set(side, present, begin):
        @pl.when(present)
        def _():
            chalo_pass(side).wait_recv()

            @pl.loop(0, 2)
            def _(i):
                set_coef(begin + i, chalo[side, i, 0], chalo[side, i, 1], chalo[side, i, 2])

            @pl.when(jnp.logical_not(first))
            def _():
                far_pass(side).wait_recv()

            a0 = chalo3[side]
            cext[side] = DIFFUSION + (jnp.maximum(a0, 0.0) if side else -jnp.minimum(a0, 0.0))

    @pl.when(odd)
    def _():
        edge_in(1, has_high)
        edge_in(0, has_low)

    @pl.when(jnp.logical_not(odd))
    def _():
        edge_in(0, has_low)
        edge_in(1, has_high)

    start_halos(False)
    edge_more(0, has_low)
    edge_more(1, has_high)
    edge_set(0, has_low, 0)
    edge_set(1, has_high, rows + 2)

    def set_hot(k):
        hit = lax.broadcasted_iota(jnp.int32, (width, LANES), 0) == obsv[k, 1, :1]
        hit = jnp.where(hit, 1.0, 0.0).astype(jnp.bfloat16)
        hot[k, :width] = hit
        hot[k, width:] = hit

    def update(c, mid, below, above):
        value = coef[c, 0] * mid
        if below is not None:
            value = value + coef[c, 1] * below
        if above is not None:
            value = value + coef[c, 2] * above
        return (
            value
            + coef[c, 3] * pltpu.roll(mid, 1, 1)
            + coef[c, 4] * pltpu.roll(mid, width - 1, 1)
            + coef[c, 5] * pltpu.roll(mid, 1, 0)
            + coef[c, 6] * pltpu.roll(mid, levels - 1, 0)
        )

    def other(d):
        return lax.rem(chip + d, chips) * 2 + core

    half = rows // 2

    def slot(src, m, h):
        return fc.at[src * members + m, pl.ds(h * half, half)]

    late = members - LAG

    def send_x(d, m, h):
        at = slot(mem, m, h)
        return remote(at, at, x_send.at[d - 1, h], x_recv.at[chips - d - 1, m, h], row, other(d))

    def from_x(d, m, h):
        at = slot(other(d), m, h)
        return remote(at, at, x_send.at[0, 0], x_recv.at[d - 1, m, h], row, other(d))

    def piece(d, m, h):
        return jnp.where(m < late, m, late + ((m - late) * chips + d) * 2 + h)

    def send_p(d, m, h):
        src = lax.rem(chip + d, chips) * 2 + core
        at = slot(src, m, h)
        return remote(at, at, p_send.at[min(d, 1)], p_recv.at[piece(d, m, h)], row, partner)

    def from_p(d, m, h):
        at = slot(lax.rem(chip + d, chips) * 2 + 1 - core, m, h)
        return remote(at, at, p_send.at[0], p_recv.at[piece(d, m, h)], row, partner)

    def from_p_whole(m):
        at = fc.at[pl.ds(0, chips)]
        return remote(at, at, p_send.at[0], p_recv.at[m], row, partner)

    def forward(m, h):
        for d in range(1, chips):
            from_x(d, m, h).wait_recv()
            send_p(d, m, h).start()

    def give(m, h):
        @pl.when(m > 0)
        def _():
            for d in range(1, chips):
                send_x(d, m - 1, h).wait_send()

        for d in range(1, chips):
            send_x(d, m, h).start()
        send_p(0, m, h).start()

        @pl.when(m >= LAG)
        def _():
            forward(m - LAG, h)

    def service(m, between):
        def source(i):
            if i < 3:
                return hal[m, 0, i]
            return ens[m, i - 3] if i < rows + 3 else hal[m, 1, i - rows - 3]

        def steps(one, two, three):
            for i in one:
                w1[i] = update(i, source(i + 1), source(i), source(i + 2))
            for i in two:
                w2[i] = update(i + 1, w1[i + 1], w1[i], w1[i + 2])
            for i in three:
                fc[mem * members + m, i] = update(i + 2, w2[i + 1], w2[i], w2[i + 2])

        @pl.when(has_low)
        def _():
            halo_up(m).wait_recv()

        @pl.when(m + ahead_up < members)
        def _():
            send_up(m + ahead_up)

        steps(range(half + 4), range(half + 2), range(half))
        give(m, 0)

        @pl.when(m == 0)
        def _():
            for n in range(FAR, RELAY):
                relay(n)

        @pl.when(m + RELAY < members)
        def _():
            relay(m + RELAY)

        between()

        @pl.when(has_high)
        def _():
            halo_down(m).wait_recv()

        @pl.when(m + ahead_down < members)
        def _():
            send_down(m + ahead_down)

        steps(range(half + 4, rows + 4), range(half + 2, rows + 2), range(half, rows))
        give(m, 1)

        @pl.when(m + DETOUR < members)
        def _():
            send_detour(m + DETOUR)

    per_pass = PER_PASS if members % PER_PASS == 0 else 1
    passes = members // per_pass

    inside = lax.broadcasted_iota(jnp.int32, (levels, LANES), 0)
    owner = lax.broadcasted_iota(jnp.int32, (levels, LANES), 1) // nobs
    pick = lax.rem(inside, TILE) == owner

    def fold(x):
        return jnp.sum(jnp.where(pick, x, 0.0).reshape(groups, TILE, LANES), axis=1)

    def profile(m, n):
        def raw(r):
            return ens[m, r] if 0 <= r < rows else None

        def first_step(r):
            return z1[r + 1] if -1 <= r <= rows else None

        def second_step(r):
            return z2[r + 2] if -2 <= r <= rows + 1 else None

        z1[0] = coef[1, 2] * raw(0)
        z1[rows + 1] = coef[rows + 2, 1] * raw(rows - 1)
        for r in range(rows):
            z1[r + 1] = update(r + 2, raw(r), raw(r - 1), raw(r + 1))
        z2[0] = coef[0, 2] * first_step(-1)
        z2[rows + 3] = coef[rows + 3, 1] * first_step(rows)
        for r in range(-1, rows + 1):
            z2[r + 2] = update(r + 2, first_step(r), first_step(r - 1), first_step(r + 1))

        def split(r, x):
            high_part = x.astype(jnp.bfloat16)
            zb[n, r + 3, :, :width] = high_part
            zb[n, r + 3, :, width:] = (x - high_part.astype(f32)).astype(jnp.bfloat16)

        split(-3, cext[0] * second_step(-2))
        split(rows + 2, cext[1] * second_step(rows + 1))
        for r in range(-2, rows + 2):
            split(r, update(r + 2, second_step(r), second_step(r - 1), second_step(r + 1)))

    def extract(begin_m):
        for k, begin, count in ((0, 3, rows), (1, 0, 3), (2, rows + 3, 3)):
            x = zb[:, pl.ds(begin, count)].reshape(per_pass * count * levels, 2 * width)
            got = jnp.dot(x, hot[k], preferred_element_type=f32)
            at = obsv[k, 0, :1] - row * rows + 3
            for n in range(per_pass):
                acc = jnp.zeros((levels, LANES), f32)
                for i in range(count):
                    base = (n * count + i) * levels
                    acc = acc + jnp.where(at == begin + i, got[base:base + levels], 0.0)
                pp[k, :, pl.ds(begin_m + n, 1)] = fold(acc)[:, None]

    def dot(a, b):
        return jnp.dot(a, b, precision=HIGHEST, preferred_element_type=f32)

    mine = pl.ds(pl.multiple_of(mem * members, members), members)

    share = total // 2

    def part_of(c):
        return pl.ds(pl.multiple_of(c * share, share), share)

    def give_low():
        return remote(pp.at[1], prec.at[1], r_send.at[1], r_recv.at[1], low, mem)

    def give_high():
        return remote(pp.at[2], prec.at[0], r_send.at[0], r_recv.at[0], high, mem)

    def stage_a():
        @pl.when(has_high)
        def _():
            give_high().start()

        @pl.when(has_low)
        def _():
            give_low().start()

    def give_prof(d):
        block = prof.at[:, mine]
        return remote(block, block, q_send.at[0], q_recv.at[0], row, lax.rem(mem + d, mem_n))

    def all_profiles():
        block = prof.at[:, pl.ds(0, (mem_n - 1) * members)]
        return remote(block, block, q_send.at[0], q_recv.at[0], row, partner)

    def stage_b():
        @pl.when(has_low)
        def _():
            give_high().wait_recv()

        @pl.when(has_high)
        def _():
            give_low().wait_recv()

        prof[:, mine] = pp[0] + prec[0] + prec[1]
        for d in range(1, mem_n):
            give_prof(d).start()

    def flat(ref):
        repeat = lax.broadcasted_iota(jnp.int32, (nobs, LANES), 1) % nobs
        repeat = jnp.where(repeat == lax.broadcasted_iota(jnp.int32, (nobs, LANES), 0), 1.0, 0.0).astype(f32)
        got = fold(dot(ref[...].T, repeat))
        return jnp.concatenate([got[q:q + 1] for q in range(groups)], axis=1)

    def give_gram(d):
        return remote(grec.at[row], grec.at[row], g_send.at[0], g_recv.at[0], lax.rem(row + d, rows_n), mem)

    def all_grams():
        block = grec.at[pl.ds(0, rows_n - 1)]
        return remote(block, block, g_send.at[0], g_recv.at[0], lax.rem(row + 1, rows_n), mem)

    def stage_c():
        all_profiles().wait_recv()
        values = jnp.concatenate([prof[q] for q in range(groups)], axis=1)
        variance = flat(obs_var)
        center = jnp.mean(values, axis=0, keepdims=True)
        scaled = (values - center) / jnp.sqrt((total - 1.0) * variance)
        innovation = (flat(obs_value) - center) / jnp.sqrt(variance)
        pad = jnp.broadcast_to(innovation, (LANES - total, innovation.shape[1]))
        scal[...] = scaled
        both = jnp.concatenate([scaled, pad], axis=0)
        grec[row] = lax.dot_general(
            scal[part_of(core)], both, (((1,), (1,)), ((), ())), precision=HIGHEST, preferred_element_type=f32
        )
        for d in range(1, rows_n):
            give_gram(d).start()

    def give_sum():
        block = gall.at[part_of(core)]
        return remote(block, block, a_send.at[0], a_recv.at[core], row, partner)

    def stage_d():
        all_grams().wait_recv()
        part = grec[0]
        for r in range(1, rows_n):
            part = part + grec[r]
        gall[part_of(core)] = part
        give_sum().start()

    def stage_e():
        block = gall.at[part_of(1 - core)]
        remote(block, block, a_send.at[0], a_recv.at[1 - core], row, partner).wait_recv()
        gsum = gall[...]
        ri = lax.broadcasted_iota(jnp.int32, (total, total), 0)
        ci = lax.broadcasted_iota(jnp.int32, (total, total), 1)
        eye = jnp.where(ri == ci, 1.0, 0.0).astype(f32)
        system = eye + gsum[:, :total]
        frob = jnp.sqrt(jnp.sum(jnp.sum(system * system, axis=1, keepdims=True), axis=0, keepdims=True))
        y = system / frob
        z = eye
        for it in range(NS_ITERS):
            factor = 0.5 * (3.0 * eye - (y if it == 0 else dot(z, y)))
            if it < NS_ITERS - 1:
                y = dot(y, factor)
            z = factor if it == 0 else dot(factor, z)
        root = z / jnp.sqrt(frob)
        shift = dot(root, dot(root, gsum))[:, total:total + 1] / jnp.sqrt(f32(total - 1.0))
        mixed = shift + root
        weights = 1.0 / total + mixed - jnp.mean(mixed, axis=0, keepdims=True)
        wts[...] = weights.T
        own = wts[mine].T
        for k in range(members):
            wsp[k] = jnp.broadcast_to(own[:, k:k + 1], (total, LANES))

    block = min(4, members)
    tiles = width // LANES

    def mix(m, h):
        @pl.when(jnp.logical_and(m < late, h == 0))
        def _():
            from_p_whole(m).wait_recv()

        @pl.when(m >= late)
        def _():
            for d in range(chips):
                from_p(d, m, h).wait_recv()

        @pl.loop(0, members // block)
        def _(b):
            ws = [
                [
                    jnp.broadcast_to(wsp[b * block + k, pl.ds(s * members + m, 1)], (TILE, LANES))
                    for s in range(mem_n)
                ]
                for k in range(block)
            ]

            @pl.loop(0, half)
            def _(n):
                i = h * half + n
                for t in range(groups):
                    for c in range(tiles):
                        at = (i, pl.ds(t * TILE, TILE), pl.ds(c * LANES, LANES))
                        f = [fc[(s * members + m,) + at] for s in range(mem_n)]
                        for k in range(block):
                            acc = out[(b * block + k,) + at]
                            for s in range(mem_n):
                                acc = acc + ws[k][s] * f[s]
                            out[(b * block + k,) + at] = acc

    at_a = passes - 1
    at_b, at_c, at_d, at_e = (min(at_a + n, members - 1) for n in STAGES)

    def profiles(group, begin, end):
        @pl.when(group < passes)
        def _():
            @pl.loop(begin, end)
            def _(n):
                profile(group * per_pass + n, n)

            if end == per_pass:
                extract(group * per_pass)

    for k in range(3):
        set_hot(k)

    @pl.loop(0, members)
    def _(m):
        service(m, lambda: profiles(m, 0, per_pass // 2))
        profiles(m, per_pass // 2, per_pass)

        for at, stage in ((at_a, stage_a), (at_b, stage_b), (at_c, stage_c), (at_d, stage_d), (at_e, stage_e)):
            pl.when(m == at)(stage)

        @pl.when(m > at_e)
        def _():
            begin = jnp.minimum(m - LAG, (m - at_e - 1) * PER_MIX)
            end = jnp.minimum(m - LAG + 1, (m - at_e) * PER_MIX)

            @pl.loop(2 * begin, 2 * end)
            def _(n):
                mix(n // 2, n % 2)

    mixed_in_loop = max(0, min(members - LAG, (members - 1 - at_e) * PER_MIX))
    @pl.loop(2 * mixed_in_loop, 2 * late)
    def _(n):
        mix(n // 2, n % 2)

    @pl.when(has_high)
    def _():
        chalo_up().wait_send()
        chalo_pass(1).wait_send()
        obs_up().wait_send()
        give_high().wait_send()
        remote(rbuf, rbuf, h_send.at[0], rb_recv.at[0], high, mem).wait_send()

        @pl.when(first)
        def _():
            far_up().wait_send()
            far_pass(1).wait_send()

    @pl.when(has_low)
    def _():
        chalo_down().wait_send()
        chalo_pass(0).wait_send()
        obs_down().wait_send()
        give_low().wait_send()
        remote(rbuf, rbuf, h_send.at[1], rb_recv.at[0], low, mem).wait_send()

        @pl.when(first)
        def _():
            far_down().wait_send()
            far_pass(0).wait_send()

    @pl.loop(0, members)
    def _(m):
        @pl.when(relays(m))
        def _():
            relay_out(m).wait_send()

    all_profiles().wait_send()
    give_sum().wait_send()
    all_grams().wait_send()

    @pl.loop(2 * late, 2 * members)
    def _(n):
        forward(n // 2, n % 2)
        mix(n // 2, n % 2)

    for h in range(2):
        for d in range(1, chips):
            send_x(d, members - 1, h).wait_send()
    for part, count in ((0, members), (1, (chips - 1) * members)):
        at = fc.at[pl.ds(0, count)]
        remote(at, at, p_send.at[part], p_recv.at[0], row, partner).wait_send()


def per_device(rows_n, mem_n, ensemble, courant, obs_column, obs_value, obs_var):
    members, levels, rows, width = ensemble.shape
    nobs = obs_column.shape[0]
    chips = mem_n // 2
    groups = levels // TILE
    f32 = jnp.float32
    vmem = pl.BlockSpec(memory_space=pltpu.VMEM)
    smem = pl.BlockSpec(memory_space=pltpu.SMEM)
    hbm = pl.BlockSpec(memory_space=pl.ANY)
    dma = pltpu.SemaphoreType.DMA
    total = members * mem_n
    plane = (levels, width)
    result = pl.pallas_call(
        functools.partial(kernel, rows_n, mem_n),
        out_shape=pltpu.VMEM((members, rows) + plane, f32),
        in_specs=[hbm, hbm, smem, vmem, vmem],
        out_specs=vmem,
        scratch_shapes=[
            pltpu.VMEM((members, rows) + plane, f32),
            pltpu.VMEM((3, rows) + plane, f32),
            pltpu.VMEM((2, 2, 3) + plane, f32),
            pltpu.VMEM((2,) + plane, f32),
            pltpu.VMEM((members, 2, 3) + plane, f32),
            pltpu.VMEM((rows + 4, 7) + plane, f32),
            pltpu.VMEM((2,) + plane, f32),
            pltpu.VMEM((rows + 4,) + plane, f32),
            pltpu.VMEM((rows + 2,) + plane, f32),
            pltpu.VMEM((rows + 2,) + plane, f32),
            pltpu.VMEM((rows + 4,) + plane, f32),
            pltpu.VMEM((PER_PASS, rows + 6, levels, 2 * width), jnp.bfloat16),
            pltpu.VMEM((members, 3) + plane, f32),
            pltpu.VMEM((total, rows) + plane, f32),
            pltpu.VMEM((3, 2, TILE, LANES), jnp.int32),
            pltpu.VMEM((3, 2 * width, LANES), jnp.bfloat16),
            pltpu.VMEM((3, groups, members, LANES), f32),
            pltpu.VMEM((2, groups, members, LANES), f32),
            pltpu.VMEM((groups, total, LANES), f32),
            pltpu.VMEM((total, groups * LANES), f32),
            pltpu.VMEM((rows_n, total // 2, LANES), f32),
            pltpu.VMEM((total, LANES), f32),
            pltpu.VMEM((total, total), f32),
            pltpu.VMEM((members, total, LANES), f32),
            dma((2,)), dma((1,)),
            dma((2,)), dma((2,)), dma((2,)), dma((2,)),
            dma((2,)), dma((2,)), dma((2,)), dma((2,)), dma((2,)), dma((2,)),
            dma((2,)), dma((2, members)), dma((members,)), dma((members,)),
            dma((chips - 1, 2)), dma((chips - 1, members, 2)), dma((2,)), dma((members - LAG + LAG * chips * 2,)),
            dma((2,)), dma((2,)),
            dma((1,)), dma((1,)),
            dma((1,)), dma((1,)),
            dma((1,)), dma((2,)),
        ],
        compiler_params=pltpu.CompilerParams(
            collective_id=0, has_side_effects=True, vmem_limit_bytes=52 * 1024 * 1024
        ),
    )(
        ensemble.transpose(0, 2, 1, 3),
        courant.transpose(0, 2, 1, 3),
        obs_column,
        obs_value.T,
        obs_var.T,
    )
    return result.transpose(0, 2, 1, 3)


def solution(mesh):
    return jax.shard_map(
        functools.partial(per_device, mesh.shape["rows"], mesh.shape["mem"]),
        mesh=mesh,
        in_specs=(
            P("mem", None, "rows", None),
            P(None, None, "rows", None),
            P("rows"),
            P(None, "rows"),
            P(None, "rows"),
        ),
        out_specs=P("mem", None, "rows", None),
        check_vma=False,
    )
```
